32 devices in a mesh: fsdp: 4 (over y, core), tp: 4 (over z), rollout: 2 (over x).
Axes of the slice: x: 2, y: 2, z: 4, core: 2. Of those that a mesh axis runs over, the one named last changes fastest.
Arguments:
- weights: bfloat16 [2, 4096, 14336], P('rollout', 'fsdp', 'tp'), may hold values from -6 to 6
- gradient: bfloat16 [2, 4096, 14336], P('rollout', 'fsdp', 'tp'), may hold values from -6 to 6
- momentum: float32 [2, 4096, 14336], P('rollout', 'fsdp', 'tp'), may hold values from -90 to 90
- basis: float32 [2, 14336, 512], P('rollout', 'tp'), may hold values from -6 to 6
Outputs:
- weights_next: bfloat16 [2, 4096, 14336], P('rollout', 'fsdp', 'tp')
- momentum_next: float32 [2, 4096, 14336], P('rollout', 'fsdp', 'tp')
- basis_next: float32 [2, 14336, 512], P('rollout', 'tp')
- rollout_weights: bfloat16 [2, 4096, 14336], P(None, 'fsdp', 'tp')
The draws below stay inside these ranges and needn't reach their ends.
All inputs are finite; a program needn't handle non-finite values.
Results may differ from the reference program's by a relative error of at most 0.013.
Values may be sent and summed in bfloat16 or wider, within the bound.
A program may use at most 192 MiB of HBM per device.

```python
import math
import jax
import jax.numpy as jnp
from jax import lax

ROWS = 4096
COLS = 14336
RANK = 512


def draw_momentum(key, part):
    key_base = jax.random.fold_in(key, 11)
    key_cols = jax.random.fold_in(key, 12)
    key_rows = jax.random.fold_in(key, 13)
    base = jnp.clip(jax.random.normal(key_base, (2, ROWS, COLS), jnp.float32), -6.0, 6.0)
    top = 10.0
    rising = jnp.exp(math.log(3.0) * jnp.arange(COLS, dtype=jnp.float32) / COLS)
    column_scale = jnp.exp(jax.random.uniform(key_cols, (2, 1, COLS), jnp.float32, 0.0, math.log(top))) * rising
    row_scale = jnp.exp(jax.random.uniform(key_rows, (2, ROWS, 1), jnp.float32, 0.0, math.log(4.0)))
    return base * column_scale * row_scale / 8.0


def level_of(rng, shape, pieces, least, top_value):
    loudness = 1.0
    for dim, shards_of in pieces:
        heights = jax.random.uniform(jax.random.fold_in(jax.random.fold_in(rng, 6), dim), (shards_of,), jnp.float32, least / len(pieces), top_value / len(pieces))
        loudness = loudness * jnp.repeat(jnp.exp(heights), shape[dim] // shards_of).reshape((-1,) + (1,) * (len(shape) - 1 - dim))
    return loudness


def scatter_about(own_key, extent, width, most, shards=(), kind=jnp.bfloat16):
    values = width * jax.random.normal(own_key, extent, jnp.float32)
    if shards:
        values = values * level_of(own_key, extent, shards, -0.22, 0.18)
    return jnp.clip(values, -most, most).astype(kind)


def setup_inputs(seed: int = 0) -> dict:
    splits = jax.random.split(jax.random.key(seed), 5)
    weights = scatter_about(splits[0], (2, ROWS, COLS), 1.0, 6.0, ((0, 2), (1, 4), (2, 4)))
    gradient = scatter_about(splits[1], (2, ROWS, COLS), 1.0, 6.0, ((0, 2), (1, 4), (2, 4)))
    momentum = draw_momentum(jax.random.fold_in(splits[4], 71), 0)
    basis = scatter_about(splits[3], (2, COLS, RANK), 1.0, 6.0, ((0, 2), (1, 4)), jnp.float32)
    return dict(weights=weights, gradient=gradient, momentum=momentum, basis=basis)


HIGH = lax.Precision.HIGHEST

def one_matrix(weight, grad, moment, prior):
    blend = moment + grad.astype(jnp.float32)
    left = jnp.dot(blend.astype(jnp.float32), prior.astype(jnp.float32), precision=HIGH, preferred_element_type=jnp.float32)
    gram = jnp.dot(left.T.astype(jnp.float32), left.astype(jnp.float32), precision=HIGH, preferred_element_type=jnp.float32)
    lower = jnp.linalg.cholesky(gram)
    ortho = lax.linalg.triangular_solve(lower, left, left_side=False, lower=True, transpose_a=True)
    right = jnp.dot(blend.T.astype(jnp.float32), ortho.astype(jnp.float32), precision=HIGH, preferred_element_type=jnp.float32)
    meansq = lax.optimization_barrier(jnp.sum(right * right, axis=0)) / COLS
    basis_new = right * lax.rsqrt(meansq + 1e-06)
    moment_new = blend - 0.05 * jnp.dot(ortho.astype(jnp.float32), right.T.astype(jnp.float32), precision=HIGH, preferred_element_type=jnp.float32)
    update = jnp.dot(ortho.astype(jnp.float32), basis_new.T.astype(jnp.float32), precision=HIGH, preferred_element_type=jnp.float32)
    weight_new = (weight.astype(jnp.float32) - 0.3 * update).astype(jnp.bfloat16)
    return (weight_new, moment_new, basis_new)

def reference(weights, gradient, momentum, basis):
    first = one_matrix(weights[0], gradient[0], momentum[0], basis[0])
    second = one_matrix(weights[1], gradient[1], momentum[1], basis[1])
    weights_next = jnp.stack([first[0], second[0]])
    momentum_next = jnp.stack([first[1], second[1]])
    basis_next = jnp.stack([first[2], second[2]])
    return (weights_next, momentum_next, basis_next, weights_next)
```

```python
import functools

import jax
import jax.numpy as jnp
from jax import lax
from jax.experimental import pallas as pl
from jax.experimental.pallas import tpu as pltpu
from jax.sharding import PartitionSpec as P


HIGH = lax.Precision.HIGHEST
BLOCK = 128
STRIP = 32
MESH = pl.DeviceIdType.MESH


def dot_t(a, b):
    return lax.dot_general(
        a, b, (((1,), (1,)), ((), ())), precision=HIGH, preferred_element_type=jnp.float32
    )


def pick(n, sizes):
    for s in sizes:
        if n % s == 0:
            return s
    return n


def remote(src, dst, send, recv, **where):
    return pltpu.make_async_remote_copy(
        src_ref=src, dst_ref=dst, send_sem=send, recv_sem=recv, device_id=where, device_id_type=MESH
    )


def greet(nf, nt):
    f, t = lax.axis_index("fsdp"), lax.axis_index("tp")
    barrier = pltpu.get_barrier_semaphore()
    n = nf * nt
    me = f * nt + t

    def one(i, carry):
        q = lax.rem(me + 1 + i, n)
        pl.semaphore_signal(
            barrier, inc=1, device_id={"fsdp": q // nt, "tp": lax.rem(q, nt)}, device_id_type=MESH
        )
        return carry

    lax.fori_loop(0, n - 1, one, 0)
    pl.semaphore_wait(barrier, n - 1)


def factor_block(s_ref, v_ref):
    nb = BLOCK
    tile = STRIP
    lane = lax.broadcasted_iota(jnp.int32, (tile, nb), 1)
    sub = lax.broadcasted_iota(jnp.int32, (tile, nb), 0)

    def strip(j, carry):
        rows = pl.ds(pl.multiple_of(j * tile, tile), tile)
        s = s_ref[rows, :]
        v = v_ref[rows, :]
        turned = pltpu.roll(s, lax.rem(nb - j * tile, nb), 1)
        cols = [jnp.broadcast_to(turned[:, i : i + 1], (tile, nb)) for i in range(tile)]
        pivot = jnp.ones((tile, nb), jnp.float32)
        recip = jnp.ones((tile, nb), jnp.float32)
        for i in range(tile):
            p = jnp.broadcast_to(cols[i][i : i + 1, :], (tile, nb))
            rp = 1.0 / p
            pivot = jnp.where(sub == i, p, pivot)
            recip = jnp.where(sub == i, rp, recip)
            if i < tile - 1:
                by = jnp.where(sub > i, cols[i] * rp, 0.0)
                for m in range(i + 1, tile):
                    cols[m] = cols[m] - by * jnp.broadcast_to(cols[m][i : i + 1, :], (tile, nb))
                s = s - by * jnp.broadcast_to(s[i : i + 1, :], (tile, nb))
                v = v - by * jnp.broadcast_to(v[i : i + 1, :], (tile, nb))
        below = jnp.where(lane >= (j + 1) * tile, s * recip, 0.0)
        change = lax.dot_general(
            below,
            jnp.concatenate([s, v], axis=1),
            (((0,), (0,)), ((), ())),
            precision=HIGH,
            preferred_element_type=jnp.float32,
        )
        s_ref[...] = s_ref[...] - change[:, :nb]
        v_ref[...] = v_ref[...] - change[:, nb:]
        r = lax.rsqrt(pivot)
        r = r * (1.5 - 0.5 * pivot * r * r)
        v_ref[rows, :] = v * r
        return carry

    lax.fori_loop(0, nb // tile, strip, 0)


def factor(a_ref, x_ref, w_ref, s_ref, v_ref):
    n = a_ref.shape[0]
    nb = BLOCK
    w_ref[...] = jnp.where(
        lax.broadcasted_iota(jnp.int32, (n, n), 0) == lax.broadcasted_iota(jnp.int32, (n, n), 1),
        1.0,
        0.0,
    ).astype(jnp.float32)
    lane = lax.broadcasted_iota(jnp.int32, (nb, nb), 1)
    sub = lax.broadcasted_iota(jnp.int32, (nb, nb), 0)

    for lo in range(0, n, nb):
        hi = lo + nb
        s_ref[...] = a_ref[lo:hi, lo:hi]
        v_ref[...] = jnp.where(lane == sub, 1.0, 0.0).astype(jnp.float32)
        factor_block(s_ref, v_ref)
        inv = v_ref[...]
        x = jnp.dot(inv, w_ref[lo:hi, :hi], precision=HIGH, preferred_element_type=jnp.float32)
        x_ref[lo:hi, :hi] = x
        if hi < n:
            x_ref[lo:hi, hi:] = jnp.zeros((nb, n - hi), jnp.float32)
            panel = dot_t(a_ref[hi:, lo:hi], inv)
            a_ref[hi:, hi:] = a_ref[hi:, hi:] - dot_t(panel, panel)
            w_ref[hi:, :hi] = w_ref[hi:, :hi] - jnp.dot(
                panel, x, precision=HIGH, preferred_element_type=jnp.float32
            )


def mid_kernel(
    nf, nt, cuts, part_ref, ortho_ref,
    left, rbuf, lbuf, gpart, gmate, pieces, gram, inverse, work, s_ref, v_ref,
    rs_send, rs_recv, mate_send, mate_recv, p_send, p_recv, q_send, q_recv, ag_send, ag_recv,
):
    f, t = lax.axis_index("fsdp"), lax.axis_index("tp")
    core = lax.rem(f, 2)
    mate = f + 1 - 2 * core
    rows, rank = part_ref.shape
    share = rows // nt
    sub = share // cuts
    half = rank // 2
    group = (nf // 2) * nt
    owners = min(group, half // 8)
    piece = half // owners
    p = (f // 2) * nt + t

    greet(nf, nt)

    def chunk(d, c):
        return part_ref.at[pl.ds(pl.multiple_of(d * share + c * sub, sub), sub)]

    def moves(i):
        c = lax.rem(i, cuts)
        k = i // cuts
        return nt - 1 - k, k, c

    def to_right(src, d, c):
        return remote(src, rbuf.at[d, c], rs_send.at[0, d, c], rs_recv.at[0, d, c], tp=t + 1)

    def to_left(src, e, c):
        return remote(src, lbuf.at[e, c], rs_send.at[1, e, c], rs_recv.at[1, e, c], tp=t - 1)

    def scatter(i, carry):
        d, e, c = moves(i)

        @pl.when(jnp.logical_and(t < d, t == 0))
        def _():
            to_right(chunk(d, c), d, c).start()

        @pl.when(jnp.logical_and(t > e, t == nt - 1))
        def _():
            to_left(chunk(e, c), e, c).start()

        @pl.when(jnp.logical_and(t < d, t > 0))
        def _():
            to_right(rbuf.at[d, c], d, c).wait_recv()
            rbuf[d, c] = rbuf[d, c] + chunk(d, c)[...]
            to_right(rbuf.at[d, c], d, c).start()

        @pl.when(jnp.logical_and(t > e, t < nt - 1))
        def _():
            to_left(lbuf.at[e, c], e, c).wait_recv()
            lbuf[e, c] = lbuf[e, c] + chunk(e, c)[...]
            to_left(lbuf.at[e, c], e, c).start()

        return carry

    lax.fori_loop(0, (nt - 1) * cuts, scatter, 0)

    def mine(c, carry):
        here = pl.ds(pl.multiple_of(t * share + c * sub, sub), sub)
        left[here, :] = part_ref[here, :]

        @pl.when(t > 0)
        def _():
            to_right(rbuf.at[t, c], t, c).wait_recv()
            left[here, :] = left[here, :] + rbuf[t, c]

        @pl.when(t < nt - 1)
        def _():
            to_left(lbuf.at[t, c], t, c).wait_recv()
            left[here, :] = left[here, :] + lbuf[t, c]

        return carry

    lax.fori_loop(0, cuts, mine, 0)

    here = pl.ds(pl.multiple_of(t * share, share), share)
    own = left[here, :]
    gpart[...] = lax.dot_general(
        own, own, (((0,), (0,)), ((), ())), precision=HIGH, preferred_element_type=jnp.float32
    )
    keep = pl.ds(pl.multiple_of(core * half, half), half)
    give = pl.ds(pl.multiple_of((1 - core) * half, half), half)
    pair = remote(gpart.at[give], gmate, mate_send.at[0], mate_recv.at[0], fsdp=mate)
    pair.start()
    pair.wait_recv()
    gmate[...] = gmate[...] + gpart[keep, :]

    def at(q):
        return {"fsdp": 2 * (q // nt) + core, "tp": lax.rem(q, nt)}

    def part_of(q):
        return gmate.at[pl.ds(pl.multiple_of(q * piece, piece), piece)]

    def send_piece(i, carry):
        q = lax.rem(p + 1 + i, group)

        @pl.when(q < owners)
        def _():
            remote(part_of(q), pieces.at[p], p_send.at[q], p_recv.at[p], **at(q)).start()

        return carry

    lax.fori_loop(0, group - 1, send_piece, 0)

    def final_of(q):
        return gram.at[pl.ds(pl.multiple_of(core * half + q * piece, piece), piece)]

    @pl.when(p < owners)
    def _():
        pieces[p] = part_of(p)[...]

        def got(i, carry):
            q = lax.rem(p + 1 + i, group)
            remote(part_of(p), pieces.at[q], p_send.at[0], p_recv.at[q], **at(q)).wait_recv()
            return carry

        lax.fori_loop(0, group - 1, got, 0)
        final_of(p)[...] = lax.fori_loop(
            1, group, lambda q, acc: acc + pieces[q], pieces[0]
        )

        def spread(i, carry):
            q = lax.rem(p + 1 + i, group)
            remote(final_of(p), final_of(p), q_send.at[q], q_recv.at[p], **at(q)).start()
            return carry

        lax.fori_loop(0, group - 1, spread, 0)

    def got_final(q, carry):
        @pl.when(q != p)
        def _():
            remote(final_of(q), final_of(q), q_send.at[0], q_recv.at[q], **at(q)).wait_recv()

        return carry

    lax.fori_loop(0, owners, got_final, 0)
    other = remote(gram.at[keep], gram.at[keep], mate_send.at[1], mate_recv.at[1], fsdp=mate)
    other.start()

    def gather(i, carry):
        q = lax.rem(t + 1 + i, nt)
        remote(left.at[here], left.at[here], ag_send.at[q], ag_recv.at[t], tp=q).start()
        return carry

    lax.fori_loop(0, nt - 1, gather, 0)
    remote(gram.at[give], gram.at[give], mate_send.at[1], mate_recv.at[1], fsdp=mate).wait_recv()
    pair.wait_send()
    gpart[...] = gram[...]
    factor(gpart, inverse, work, s_ref, v_ref)

    def ortho_of(i, carry):
        q = lax.rem(t + i, nt)
        there = pl.ds(pl.multiple_of(q * share, share), share)

        @pl.when(i > 0)
        def _():
            remote(left.at[there], left.at[there], ag_send.at[0], ag_recv.at[q], tp=q).wait_recv()

        ortho_ref[there, :] = dot_t(left[there, :], inverse[...]).astype(jnp.bfloat16)
        return carry

    lax.fori_loop(0, nt, ortho_of, 0)

    def drain(i, carry):
        d, e, c = moves(i)

        @pl.when(t < d)
        def _():
            to_right(rbuf.at[d, c], d, c).wait_send()

        @pl.when(t > e)
        def _():
            to_left(lbuf.at[e, c], e, c).wait_send()

        return carry

    lax.fori_loop(0, (nt - 1) * cuts, drain, 0)
    other.wait_send()

    def drain_pieces(i, carry):
        q = lax.rem(p + 1 + i, group)

        @pl.when(q < owners)
        def _():
            remote(part_of(q), pieces.at[p], p_send.at[q], p_recv.at[p], **at(q)).wait_send()

        @pl.when(p < owners)
        def _():
            remote(final_of(p), final_of(p), q_send.at[q], q_recv.at[p], **at(q)).wait_send()

        return carry

    lax.fori_loop(0, group - 1, drain_pieces, 0)

    def drain_gather(i, carry):
        q = lax.rem(t + 1 + i, nt)
        remote(left.at[here], left.at[here], ag_send.at[q], ag_recv.at[t], tp=q).wait_send()
        return carry

    lax.fori_loop(0, nt - 1, drain_gather, 0)


def mid(part, nf, nt):
    rows, rank = part.shape
    share = rows // nt
    cuts = 2 if (share // 2) % 8 == 0 else 1
    sub = share // cuts
    half = rank // 2
    group = (nf // 2) * nt
    owners = min(group, half // 8)
    f32 = jnp.float32
    dma = pltpu.SemaphoreType.DMA
    return pl.pallas_call(
        functools.partial(mid_kernel, nf, nt, cuts),
        out_shape=jax.ShapeDtypeStruct((rows, rank), jnp.bfloat16),
        in_specs=[pl.BlockSpec(memory_space=pltpu.VMEM)],
        out_specs=pl.BlockSpec(memory_space=pltpu.VMEM),
        scratch_shapes=[
            pltpu.VMEM((rows, rank), f32),
            pltpu.VMEM((nt, cuts, sub, rank), f32),
            pltpu.VMEM((nt, cuts, sub, rank), f32),
            pltpu.VMEM((rank, rank), f32),
            pltpu.VMEM((half, rank), f32),
            pltpu.VMEM((group, half // owners, rank), f32),
            pltpu.VMEM((rank, rank), f32),
            pltpu.VMEM((rank, rank), f32),
            pltpu.VMEM((rank, rank), f32),
            pltpu.VMEM((BLOCK, BLOCK), f32),
            pltpu.VMEM((BLOCK, BLOCK), f32),
            dma((2, nt, cuts)), dma((2, nt, cuts)),
            dma((2,)), dma((2,)),
            dma((group,)), dma((group,)),
            dma((group,)), dma((group,)),
            dma((nt,)), dma((nt,)),
        ],
        compiler_params=pltpu.CompilerParams(
            vmem_limit_bytes=40 << 20, collective_id=0, has_side_effects=True
        ),
        cost_estimate=pl.CostEstimate(
            flops=30_000_000_000, bytes_accessed=8 * rank * rank, transcendentals=0
        ),
        name="mid",
    )(part)


def right_kernel(
    nf, nt, cuts, cols, part_ref, right_ref, inv_ref,
    mbuf, sbuf, ybuf, sqs,
    m_send, m_recv, y_send, y_recv, g_send, g_recv, w_send, w_recv, sq_send, sq_recv,
):
    f, t = lax.axis_index("fsdp"), lax.axis_index("tp")
    core = lax.rem(f, 2)
    y = f // 2
    ny = nf // 2
    mate = f + 1 - 2 * core
    half = part_ref.shape[0] // 2
    quarter = half // ny
    sub = quarter // cuts
    n = nf * nt
    me = f * nt + t
    f32, b16 = jnp.float32, jnp.bfloat16

    greet(nf, nt)

    def rows_of(h, q, c):
        return pl.ds(pl.multiple_of(h * half + q * quarter + c * sub, sub), sub)

    def order(i):
        return lax.rem(y + 1 + i // cuts, ny), lax.rem(i, cuts)

    def to_mate(q, c):
        return remote(
            part_ref.at[rows_of(1 - core, q, c)], mbuf.at[q, c], m_send.at[q, c], m_recv.at[q, c],
            fsdp=mate,
        )

    def start_mate(i, carry):
        q, c = order(i)
        to_mate(q, c).start()
        return carry

    lax.fori_loop(0, ny * cuts, start_mate, 0)

    def to_peer(q, c):
        return remote(
            sbuf.at[q, c], ybuf.at[y, c], y_send.at[q, c], y_recv.at[y, c], fsdp=2 * q + core
        )

    def pair_sum(i, carry):
        q, c = order(i)
        to_mate(q, c).wait_recv()
        sbuf[q, c] = (part_ref[rows_of(core, q, c), :].astype(f32) + mbuf[q, c].astype(f32)).astype(b16)
        to_peer(q, c).start()
        return carry

    lax.fori_loop(0, (ny - 1) * cuts, pair_sum, 0)

    def spread(q, c):
        rows = rows_of(core, y, c)
        return remote(
            right_ref.at[rows], right_ref.at[rows], g_send.at[q, c], g_recv.at[y, c], fsdp=2 * q + core
        )

    def to_other_core(q, c):
        rows = rows_of(core, q, c)
        return remote(
            right_ref.at[rows], right_ref.at[rows], w_send.at[q, c], w_recv.at[q, c], fsdp=mate
        )

    sqs[me] = jnp.zeros_like(sqs[me])

    def reduce(c, carry):
        to_mate(y, c).wait_recv()
        total = part_ref[rows_of(core, y, c), :].astype(f32) + mbuf[y, c].astype(f32)

        def add(i, acc):
            q = lax.rem(y + 1 + i, ny)
            remote(
                sbuf.at[y, c], ybuf.at[q, c], y_send.at[q, c], y_recv.at[q, c], fsdp=2 * q + core
            ).wait_recv()
            return acc + ybuf[q, c].astype(f32)

        total = lax.fori_loop(0, ny - 1, add, total)
        rows = rows_of(core, y, c)
        right_ref[rows, :] = total.astype(b16)
        sqs[me] = sqs[me] + jnp.sum((total * total).reshape(sub // 8, 8, total.shape[1]), axis=0)

        def send(i, carry):
            spread(lax.rem(y + 1 + i, ny), c).start()
            return carry

        lax.fori_loop(0, ny - 1, send, 0)
        to_other_core(y, c).start()
        return carry

    lax.fori_loop(0, cuts, reduce, 0)

    def to_all(q):
        return remote(
            sqs.at[me], sqs.at[me], sq_send.at[q], sq_recv.at[me], fsdp=q // nt, tp=lax.rem(q, nt)
        )

    def start_squares(i, carry):
        to_all(lax.rem(me + 1 + i, n)).start()
        return carry

    lax.fori_loop(0, n - 1, start_squares, 0)

    def forward(i, carry):
        q, c = order(i)
        rows = rows_of(core, q, c)
        remote(
            right_ref.at[rows], right_ref.at[rows], g_send.at[q, c], g_recv.at[q, c], fsdp=2 * q + core
        ).wait_recv()
        to_other_core(q, c).start()
        return carry

    lax.fori_loop(0, (ny - 1) * cuts, forward, 0)

    def got_square(i, carry):
        q = lax.rem(me + 1 + i, n)
        remote(
            sqs.at[q], sqs.at[q], sq_send.at[q], sq_recv.at[q], fsdp=q // nt, tp=lax.rem(q, nt)
        ).wait_recv()
        return carry

    lax.fori_loop(0, n - 1, got_square, 0)
    total = lax.fori_loop(1, n, lambda q, acc: acc + sqs[q], sqs[0])
    meansq = jnp.sum(total, axis=0, keepdims=True) / cols
    inv_ref[...] = lax.rsqrt(meansq + 1e-06)

    def finish(i, carry):
        q, c = order(i)
        rows = rows_of(1 - core, q, c)
        remote(
            right_ref.at[rows], right_ref.at[rows], w_send.at[q, c], w_recv.at[q, c], fsdp=mate
        ).wait_recv()
        to_mate(q, c).wait_send()
        to_other_core(q, c).wait_send()

        @pl.when(q != y)
        def _():
            to_peer(q, c).wait_send()
            spread(q, c).wait_send()

        return carry

    lax.fori_loop(0, ny * cuts, finish, 0)

    def drain_squares(i, carry):
        to_all(lax.rem(me + 1 + i, n)).wait_send()
        return carry

    lax.fori_loop(0, n - 1, drain_squares, 0)


def sub_blocks(quarter):
    for cuts in (4, 2):
        if quarter % (16 * cuts) == 0:
            return cuts
    return 1


def right_sum(part, nf, nt, cols):
    mine, rank = part.shape
    ny = nf // 2
    quarter = mine // nf
    cuts = sub_blocks(quarter)
    sub = quarter // cuts
    n = nf * nt
    b16 = jnp.bfloat16
    dma = pltpu.SemaphoreType.DMA
    return pl.pallas_call(
        functools.partial(right_kernel, nf, nt, cuts, cols),
        out_shape=(
            jax.ShapeDtypeStruct((mine, rank), b16),
            jax.ShapeDtypeStruct((1, rank), jnp.float32),
        ),
        in_specs=[pl.BlockSpec(memory_space=pltpu.VMEM)],
        out_specs=(pl.BlockSpec(memory_space=pltpu.VMEM), pl.BlockSpec(memory_space=pltpu.VMEM)),
        scratch_shapes=[
            pltpu.VMEM((ny, cuts, sub, rank), b16),
            pltpu.VMEM((ny, cuts, sub, rank), b16),
            pltpu.VMEM((ny, cuts, sub, rank), b16),
            pltpu.VMEM((n, 8, rank), jnp.float32),
            dma((ny, cuts)), dma((ny, cuts)),
            dma((ny, cuts)), dma((ny, cuts)),
            dma((ny, cuts)), dma((ny, cuts)),
            dma((ny, cuts)), dma((ny, cuts)),
            dma((n,)), dma((n,)),
        ],
        compiler_params=pltpu.CompilerParams(
            vmem_limit_bytes=40 << 20, collective_id=1, has_side_effects=True
        ),
        cost_estimate=pl.CostEstimate(
            flops=10_000_000_000, bytes_accessed=4 * mine * rank, transcendentals=0
        ),
        name="right_sum",
    )(part)


def spread_kernel(
    nf, nt, cuts, o_ref, r_ref, ortho_ref, right_ref,
    o_send, o_recv, g_send, g_recv, w_send, w_recv, here_sem,
):
    f, t = lax.axis_index("fsdp"), lax.axis_index("tp")
    core = lax.rem(f, 2)
    y = f // 2
    ny = nf // 2
    mate = f + 1 - 2 * core
    share = o_ref.shape[0]
    quarter = r_ref.shape[0]
    half = quarter * ny
    sub = quarter // cuts

    greet(nf, nt)

    def rows_of(h, q, c):
        return pl.ds(pl.multiple_of(h * half + q * quarter + c * sub, sub), sub)

    def mine(c):
        return r_ref.at[pl.ds(pl.multiple_of(c * sub, sub), sub)]

    def block(q):
        return pl.ds(pl.multiple_of(q * share, share), share)

    def order(i):
        return lax.rem(y + 1 + i // cuts, ny), lax.rem(i, cuts)

    def to_peer(q, c):
        return remote(
            mine(c), right_ref.at[rows_of(core, y, c)], g_send.at[q, c], g_recv.at[y, c],
            fsdp=2 * q + core,
        )

    def start_peer(i, carry):
        q, c = order(i)
        to_peer(q, c).start()
        return carry

    lax.fori_loop(0, (ny - 1) * cuts, start_peer, 0)

    def to_line(q):
        return remote(o_ref, ortho_ref.at[block(t)], o_send.at[q], o_recv.at[t], tp=q)

    def start_line(i, carry):
        to_line(lax.rem(t + 1 + i, nt)).start()
        return carry

    lax.fori_loop(0, nt - 1, start_line, 0)

    def own_to_mate(c):
        return remote(
            mine(c), right_ref.at[rows_of(core, y, c)], w_send.at[y, c], w_recv.at[y, c], fsdp=mate
        )

    def start_own(c, carry):
        own_to_mate(c).start()
        return carry

    lax.fori_loop(0, cuts, start_own, 0)
    first = pltpu.make_async_copy(o_ref, ortho_ref.at[block(t)], here_sem.at[0])
    second = pltpu.make_async_copy(
        r_ref, right_ref.at[pl.ds(pl.multiple_of(core * half + y * quarter, quarter), quarter)], here_sem.at[1]
    )
    first.start()
    second.start()

    def to_other_core(q, c):
        rows = rows_of(core, q, c)
        return remote(
            right_ref.at[rows], right_ref.at[rows], w_send.at[q, c], w_recv.at[q, c], fsdp=mate
        )

    def forward(i, carry):
        q, c = order(i)
        rows = rows_of(core, q, c)
        remote(mine(c), right_ref.at[rows], g_send.at[q, c], g_recv.at[q, c], fsdp=2 * q + core).wait_recv()
        to_other_core(q, c).start()
        return carry

    lax.fori_loop(0, (ny - 1) * cuts, forward, 0)

    def finish(i, carry):
        q, c = order(i)
        rows = rows_of(1 - core, q, c)
        remote(
            right_ref.at[rows], right_ref.at[rows], w_send.at[q, c], w_recv.at[q, c], fsdp=mate
        ).wait_recv()
        to_other_core(q, c).wait_send()

        @pl.when(q != y)
        def _():
            to_peer(q, c).wait_send()

        return carry

    lax.fori_loop(0, ny * cuts, finish, 0)

    def finish_line(i, carry):
        q = lax.rem(t + 1 + i, nt)
        remote(o_ref, ortho_ref.at[block(q)], o_send.at[q], o_recv.at[q], tp=q).wait_recv()
        to_line(q).wait_send()
        return carry

    lax.fori_loop(0, nt - 1, finish_line, 0)
    first.wait()
    second.wait()


def spread_other(ortho, right, nf, nt):
    share, rank = ortho.shape
    quarter = right.shape[0]
    ny = nf // 2
    cuts = sub_blocks(quarter)
    dma = pltpu.SemaphoreType.DMA
    vmem = pl.BlockSpec(memory_space=pltpu.VMEM)
    return pl.pallas_call(
        functools.partial(spread_kernel, nf, nt, cuts),
        out_shape=(
            jax.ShapeDtypeStruct((share * nt, rank), jnp.bfloat16),
            jax.ShapeDtypeStruct((quarter * nf, rank), jnp.bfloat16),
        ),
        in_specs=[vmem, vmem],
        out_specs=(vmem, vmem),
        scratch_shapes=[
            dma((nt,)), dma((nt,)),
            dma((ny, cuts)), dma((ny, cuts)),
            dma((ny, cuts)), dma((ny, cuts)),
            dma((2,)),
        ],
        compiler_params=pltpu.CompilerParams(
            vmem_limit_bytes=32 << 20, collective_id=2, has_side_effects=True
        ),
        cost_estimate=pl.CostEstimate(
            flops=5_000_000_000, bytes_accessed=4 * quarter * nf * rank, transcendentals=0
        ),
        name="spread_other",
    )(ortho, right)


def updated(w_ref, ortho_ref, right_ref, inv_ref):
    base = (right_ref[...].astype(jnp.float32) * inv_ref[...]).astype(jnp.bfloat16)
    update = lax.dot_general(
        ortho_ref[...], base, (((1,), (1,)), ((), ())), preferred_element_type=jnp.float32
    )
    return (w_ref[0].astype(jnp.float32) - 0.3 * update).astype(jnp.bfloat16)


def own_kernel(who_ref, w_ref, ortho_ref, right_ref, inv_ref, new_ref, both_ref):
    value = updated(w_ref, ortho_ref, right_ref, inv_ref)
    new_ref[0] = value
    both_ref[0] = value


def other_kernel(who_ref, w_ref, ortho_ref, right_ref, inv_ref, both_in, both_ref):
    both_ref[0] = updated(w_ref, ortho_ref, right_ref, inv_ref)


def apply_update(who, w, ortho, right, inv, both=None):
    _, rows, cols = w.shape
    rank = ortho.shape[1]
    tr = pick(rows, (512, 256, 128))
    tc = pick(cols, (896, 512, 256, 128))
    w_spec = pl.BlockSpec((1, tr, tc), lambda j, i, who: (0, i, j))
    both_spec = pl.BlockSpec((1, tr, tc), lambda j, i, who: (who[0], i, j))
    in_specs = [
        w_spec,
        pl.BlockSpec((tr, rank), lambda j, i, who: (i, 0)),
        pl.BlockSpec((tc, rank), lambda j, i, who: (j, 0)),
        pl.BlockSpec((1, rank), lambda j, i, who: (0, 0)),
    ]
    both_shape = jax.ShapeDtypeStruct((2, rows, cols), jnp.bfloat16)
    args = [who, w, ortho, right, inv]
    if both is None:
        kernel = own_kernel
        out_shape = (jax.ShapeDtypeStruct((1, rows, cols), jnp.bfloat16), both_shape)
        out_specs = (w_spec, both_spec)
        aliases = {}
    else:
        kernel = other_kernel
        in_specs.append(pl.BlockSpec(memory_space=pl.ANY))
        args.append(both)
        out_shape = both_shape
        out_specs = both_spec
        aliases = {5: 0}
    return pl.pallas_call(
        kernel,
        out_shape=out_shape,
        grid_spec=pltpu.PrefetchScalarGridSpec(
            num_scalar_prefetch=1,
            grid=(cols // tc, rows // tr),
            in_specs=in_specs,
            out_specs=out_specs,
        ),
        input_output_aliases=aliases,
        compiler_params=pltpu.CompilerParams(vmem_limit_bytes=32 << 20),
        cost_estimate=pl.CostEstimate(
            flops=2 * rows * cols * rank, bytes_accessed=6 * rows * cols, transcendentals=0
        ),
        name="apply_own" if both is None else "apply_other",
    )(*args)


def body(weights, gradient, momentum, basis):
    swap = functools.partial(lax.ppermute, axis_name="rollout", perm=[(0, 1), (1, 0)])
    me = lax.axis_index("rollout")
    f, t = lax.axis_index("fsdp"), lax.axis_index("tp")
    nf, nt = lax.axis_size("fsdp"), lax.axis_size("tp")
    cols = weights.shape[2] * nt
    weights_other = swap(weights)
    blend = momentum[0] + gradient[0].astype(jnp.float32)
    part = jnp.dot(blend, basis[0], precision=HIGH, preferred_element_type=jnp.float32)
    ortho = mid(part, nf, nt)
    rows = ortho.shape[0]
    partial_right = lax.dot_general(
        blend.astype(jnp.bfloat16),
        ortho,
        (((0,), (0,)), ((), ())),
        preferred_element_type=jnp.float32,
    ).astype(jnp.bfloat16)
    right, inv = right_sum(partial_right, nf, nt, cols)
    share = rows // nt
    quarter = right.shape[0] // nf
    ortho_piece = swap(lax.dynamic_slice_in_dim(ortho, t * share, share, 0))
    place = (f % 2) * (nf // 2) + f // 2
    right_piece = swap(lax.dynamic_slice_in_dim(right, place * quarter, quarter, 0))
    inv_other = swap(inv)
    weight_new, both = apply_update(me.reshape(1), weights, ortho, right, inv)
    moment_new = blend - 0.05 * lax.dot_general(
        ortho, right, (((1,), (1,)), ((), ())), preferred_element_type=jnp.float32
    )
    basis_new = right.astype(jnp.float32) * inv
    ortho_other, right_other = spread_other(ortho_piece, right_piece, nf, nt)
    both = apply_update((1 - me).reshape(1), weights_other, ortho_other, right_other, inv_other, both)
    return (weight_new, moment_new[None], basis_new[None], both)


def solution(mesh):
    return jax.shard_map(
        body,
        mesh=mesh,
        in_specs=(
            P("rollout", "fsdp", "tp"),
            P("rollout", "fsdp", "tp"),
            P("rollout", "fsdp", "tp"),
            P("rollout", "tp", None),
        ),
        out_specs=(
            P("rollout", "fsdp", "tp"),
            P("rollout", "fsdp", "tp"),
            P("rollout", "tp", None),
            P(None, "fsdp", "tp"),
        ),
        check_vma=False,
    )
```

```python
import functools

import jax
import jax.numpy as jnp
from jax import lax
from jax.experimental import pallas as pl
from jax.experimental.pallas import tpu as pltpu
from jax.sharding import PartitionSpec as P


HIGH = lax.Precision.HIGHEST
BLOCK = 128
STRIP = 32
MESH = pl.DeviceIdType.MESH


def dot_t(a, b):
    return lax.dot_general(
        a, b, (((1,), (1,)), ((), ())), precision=HIGH, preferred_element_type=jnp.float32
    )


def pick(n, sizes):
    for s in sizes:
        if n % s == 0:
            return s
    return n


def remote(src, dst, send, recv, **where):
    return pltpu.make_async_remote_copy(
        src_ref=src, dst_ref=dst, send_sem=send, recv_sem=recv, device_id=where, device_id_type=MESH
    )


def greet(nf, nt, across=False):
    f, t = lax.axis_index("fsdp"), lax.axis_index("tp")
    barrier = pltpu.get_barrier_semaphore()
    n = nf * nt
    me = f * nt + t

    def one(i, carry):
        q = lax.rem(me + 1 + i, n)
        pl.semaphore_signal(
            barrier, inc=1, device_id={"fsdp": q // nt, "tp": lax.rem(q, nt)}, device_id_type=MESH
        )
        return carry

    lax.fori_loop(0, n - 1, one, 0)
    if across:
        pl.semaphore_signal(
            barrier, inc=1, device_id={"rollout": 1 - lax.axis_index("rollout")}, device_id_type=MESH
        )
    pl.semaphore_wait(barrier, n - 1 + across)


def factor_block(s_ref, v_ref):
    nb = BLOCK
    tile = STRIP
    lane = lax.broadcasted_iota(jnp.int32, (tile, nb), 1)
    sub = lax.broadcasted_iota(jnp.int32, (tile, nb), 0)

    def strip(j, carry):
        rows = pl.ds(pl.multiple_of(j * tile, tile), tile)
        s = s_ref[rows, :]
        v = v_ref[rows, :]
        turned = pltpu.roll(s, lax.rem(nb - j * tile, nb), 1)
        cols = [jnp.broadcast_to(turned[:, i : i + 1], (tile, nb)) for i in range(tile)]
        pivot = jnp.ones((tile, nb), jnp.float32)
        recip = jnp.ones((tile, nb), jnp.float32)
        for i in range(tile):
            p = jnp.broadcast_to(cols[i][i : i + 1, :], (tile, nb))
            rp = 1.0 / p
            pivot = jnp.where(sub == i, p, pivot)
            recip = jnp.where(sub == i, rp, recip)
            if i < tile - 1:
                by = jnp.where(sub > i, cols[i] * rp, 0.0)
                for m in range(i + 1, tile):
                    cols[m] = cols[m] - by * jnp.broadcast_to(cols[m][i : i + 1, :], (tile, nb))
                s = s - by * jnp.broadcast_to(s[i : i + 1, :], (tile, nb))
                v = v - by * jnp.broadcast_to(v[i : i + 1, :], (tile, nb))
        below = jnp.where(lane >= (j + 1) * tile, s * recip, 0.0)
        change = lax.dot_general(
            below,
            jnp.concatenate([s, v], axis=1),
            (((0,), (0,)), ((), ())),
            precision=HIGH,
            preferred_element_type=jnp.float32,
        )
        s_ref[...] = s_ref[...] - change[:, :nb]
        v_ref[...] = v_ref[...] - change[:, nb:]
        r = lax.rsqrt(pivot)
        r = r * (1.5 - 0.5 * pivot * r * r)
        v_ref[rows, :] = v * r
        return carry

    lax.fori_loop(0, nb // tile, strip, 0)


def factor(a_ref, x_ref, w_ref, s_ref, v_ref):
    n = a_ref.shape[0]
    nb = BLOCK
    w_ref[...] = jnp.where(
        lax.broadcasted_iota(jnp.int32, (n, n), 0) == lax.broadcasted_iota(jnp.int32, (n, n), 1),
        1.0,
        0.0,
    ).astype(jnp.float32)
    lane = lax.broadcasted_iota(jnp.int32, (nb, nb), 1)
    sub = lax.broadcasted_iota(jnp.int32, (nb, nb), 0)

    for lo in range(0, n, nb):
        hi = lo + nb
        s_ref[...] = a_ref[lo:hi, lo:hi]
        v_ref[...] = jnp.where(lane == sub, 1.0, 0.0).astype(jnp.float32)
        factor_block(s_ref, v_ref)
        inv = v_ref[...]
        x = jnp.dot(inv, w_ref[lo:hi, :hi], precision=HIGH, preferred_element_type=jnp.float32)
        x_ref[lo:hi, :hi] = x
        if hi < n:
            x_ref[lo:hi, hi:] = jnp.zeros((nb, n - hi), jnp.float32)
            panel = dot_t(a_ref[hi:, lo:hi], inv)
            a_ref[hi:, hi:] = a_ref[hi:, hi:] - dot_t(panel, panel)
            w_ref[hi:, :hi] = w_ref[hi:, :hi] - jnp.dot(
                panel, x, precision=HIGH, preferred_element_type=jnp.float32
            )


def mid_kernel(
    nf, nt, cuts, moment_ref, grad_ref, basis_ref, ortho_ref,
    part_ref, high, low, basis_stage, moment_stage, grad_stage, in_sem, left, rbuf, lbuf, gpart, gmate, pieces, gram, inverse, work, s_ref, v_ref,
    rs_send, rs_recv, mate_send, mate_recv, p_send, p_recv, q_send, q_recv, ag_send, ag_recv,
):
    f, t = lax.axis_index("fsdp"), lax.axis_index("tp")
    core = lax.rem(f, 2)
    mate = f + 1 - 2 * core
    rows, rank = part_ref.shape
    share = rows // nt
    sub = share // cuts
    half = rank // 2
    bits = basis_stage.shape[1]
    pieces_of_basis = high.shape[0] // bits
    f32, b16 = jnp.float32, jnp.bfloat16

    def block_at(i):
        k = jnp.where(lax.rem(i, 2) == 0, nt - 1 - i // 2, i // 2)
        return jnp.where(t < (nt + 1) // 2, k, nt - 1 - k)

    def fetch_rows(i):
        where = pl.ds(pl.multiple_of(block_at(i) * share, share), share)
        slot = lax.rem(i, 2)
        return (
            pltpu.make_async_copy(moment_ref.at[0, where], moment_stage.at[slot], in_sem.at[slot]),
            pltpu.make_async_copy(grad_ref.at[0, where], grad_stage.at[slot], in_sem.at[2 + slot]),
        )

    def fetch_basis(i):
        where = pl.ds(pl.multiple_of(i * bits, bits), bits)
        slot = lax.rem(i, 2)
        return pltpu.make_async_copy(basis_ref.at[0, where], basis_stage.at[slot], in_sem.at[4 + slot])

    fetch_basis(0).start()
    for copy in fetch_rows(0):
        copy.start()
    group = (nf // 2) * nt
    owners = min(group, half // 8)
    piece = half // owners
    p = (f // 2) * nt + t

    greet(nf, nt)

    def chunk(d, c):
        return part_ref.at[pl.ds(pl.multiple_of(d * share + c * sub, sub), sub)]

    def moves(i):
        c = lax.rem(i, cuts)
        k = i // cuts
        return nt - 1 - k, k, c

    def to_right(src, d, c):
        return remote(src, rbuf.at[d, c], rs_send.at[0, d, c], rs_recv.at[0, d, c], tp=t + 1)

    def to_left(src, e, c):
        return remote(src, lbuf.at[e, c], rs_send.at[1, e, c], rs_recv.at[1, e, c], tp=t - 1)

    def split_basis(i, carry):
        fetch_basis(i).wait()

        @pl.when(i + 1 < pieces_of_basis)
        def _():
            fetch_basis(i + 1).start()

        value = basis_stage[lax.rem(i, 2)]
        where = pl.ds(pl.multiple_of(i * bits, bits), bits)
        top = value.astype(b16)
        high[where, :] = top
        low[where, :] = (value - top.astype(f32)).astype(b16)
        return carry

    lax.fori_loop(0, pieces_of_basis, split_basis, 0)

    def left_block(i, carry):
        slot = lax.rem(i, 2)
        for copy in fetch_rows(i):
            copy.wait()

        @pl.when(i + 1 < nt)
        def _():
            for copy in fetch_rows(i + 1):
                copy.start()

        d = block_at(i)
        value = moment_stage[slot] + grad_stage[slot].astype(f32)
        top = value.astype(b16)
        rest = (value - top.astype(f32)).astype(b16)
        part_ref[pl.ds(pl.multiple_of(d * share, share), share), :] = (
            jnp.dot(top, low[...], preferred_element_type=f32)
            + jnp.dot(rest, high[...], preferred_element_type=f32)
            + jnp.dot(top, high[...], preferred_element_type=f32)
        )

        def begin(c, inner):
            @pl.when(jnp.logical_and(t == 0, d > 0))
            def _():
                to_right(chunk(d, c), d, c).start()

            @pl.when(jnp.logical_and(t == nt - 1, d < nt - 1))
            def _():
                to_left(chunk(d, c), d, c).start()

            return inner

        lax.fori_loop(0, cuts, begin, 0)
        return carry

    lax.fori_loop(0, nt, left_block, 0)

    def scatter(i, carry):
        d, e, c = moves(i)

        @pl.when(jnp.logical_and(t < d, t > 0))
        def _():
            to_right(rbuf.at[d, c], d, c).wait_recv()
            rbuf[d, c] = rbuf[d, c] + chunk(d, c)[...]
            to_right(rbuf.at[d, c], d, c).start()

        @pl.when(jnp.logical_and(t > e, t < nt - 1))
        def _():
            to_left(lbuf.at[e, c], e, c).wait_recv()
            lbuf[e, c] = lbuf[e, c] + chunk(e, c)[...]
            to_left(lbuf.at[e, c], e, c).start()

        return carry

    lax.fori_loop(0, (nt - 1) * cuts, scatter, 0)

    def mine(c, carry):
        here = pl.ds(pl.multiple_of(t * share + c * sub, sub), sub)
        left[here, :] = part_ref[here, :]

        @pl.when(t > 0)
        def _():
            to_right(rbuf.at[t, c], t, c).wait_recv()
            left[here, :] = left[here, :] + rbuf[t, c]

        @pl.when(t < nt - 1)
        def _():
            to_left(lbuf.at[t, c], t, c).wait_recv()
            left[here, :] = left[here, :] + lbuf[t, c]

        return carry

    lax.fori_loop(0, cuts, mine, 0)

    here = pl.ds(pl.multiple_of(t * share, share), share)
    own = left[here, :]
    gpart[...] = lax.dot_general(
        own, own, (((0,), (0,)), ((), ())), precision=HIGH, preferred_element_type=jnp.float32
    )
    keep = pl.ds(pl.multiple_of(core * half, half), half)
    give = pl.ds(pl.multiple_of((1 - core) * half, half), half)
    pair = remote(gpart.at[give], gmate, mate_send.at[0], mate_recv.at[0], fsdp=mate)
    pair.start()
    pair.wait_recv()
    gmate[...] = gmate[...] + gpart[keep, :]

    def at(q):
        return {"fsdp": 2 * (q // nt) + core, "tp": lax.rem(q, nt)}

    def part_of(q):
        return gmate.at[pl.ds(pl.multiple_of(q * piece, piece), piece)]

    def send_piece(i, carry):
        q = lax.rem(p + 1 + i, group)

        @pl.when(q < owners)
        def _():
            remote(part_of(q), pieces.at[p], p_send.at[q], p_recv.at[p], **at(q)).start()

        return carry

    lax.fori_loop(0, group - 1, send_piece, 0)

    def final_of(q):
        return gram.at[pl.ds(pl.multiple_of(core * half + q * piece, piece), piece)]

    @pl.when(p < owners)
    def _():
        pieces[p] = part_of(p)[...]

        def got(i, carry):
            q = lax.rem(p + 1 + i, group)
            remote(part_of(p), pieces.at[q], p_send.at[0], p_recv.at[q], **at(q)).wait_recv()
            return carry

        lax.fori_loop(0, group - 1, got, 0)
        final_of(p)[...] = lax.fori_loop(
            1, group, lambda q, acc: acc + pieces[q], pieces[0]
        )

        def spread(i, carry):
            q = lax.rem(p + 1 + i, group)
            remote(final_of(p), final_of(p), q_send.at[q], q_recv.at[p], **at(q)).start()
            return carry

        lax.fori_loop(0, group - 1, spread, 0)

    def got_final(q, carry):
        @pl.when(q != p)
        def _():
            remote(final_of(q), final_of(q), q_send.at[0], q_recv.at[q], **at(q)).wait_recv()

        return carry

    lax.fori_loop(0, owners, got_final, 0)
    other = remote(gram.at[keep], gram.at[keep], mate_send.at[1], mate_recv.at[1], fsdp=mate)
    other.start()

    def near(q):
        return jnp.logical_or(q == t + 1, q == t - 1)

    def give_left(q):
        return remote(left.at[here], left.at[here], ag_send.at[q], ag_recv.at[t], tp=q)

    def give_ortho(q):
        return remote(ortho_ref.at[here], ortho_ref.at[here], ag_send.at[q], ag_recv.at[t], tp=q)

    def gather(i, carry):
        q = lax.rem(t + 1 + i, nt)

        @pl.when(near(q))
        def _():
            give_left(q).start()

        return carry

    lax.fori_loop(0, nt - 1, gather, 0)
    remote(gram.at[give], gram.at[give], mate_send.at[1], mate_recv.at[1], fsdp=mate).wait_recv()
    pair.wait_send()
    gpart[...] = gram[...]
    factor(gpart, inverse, work, s_ref, v_ref)

    inv_high = inverse[...].astype(b16)
    inv_low = (inverse[...] - inv_high.astype(f32)).astype(b16)

    def ortho_of(i, carry):
        q = lax.rem(t + i, nt)
        there = pl.ds(pl.multiple_of(q * share, share), share)

        @pl.when(near(q))
        def _():
            remote(left.at[there], left.at[there], ag_send.at[0], ag_recv.at[q], tp=q).wait_recv()

        @pl.when(jnp.logical_or(i == 0, near(q)))
        def _():
            value = left[there, :]
            top = value.astype(b16)
            rest = (value - top.astype(f32)).astype(b16)
            dims = (((1,), (1,)), ((), ()))
            ortho_ref[there, :] = (
                lax.dot_general(top, inv_low, dims, preferred_element_type=f32)
                + lax.dot_general(rest, inv_high, dims, preferred_element_type=f32)
                + lax.dot_general(top, inv_high, dims, preferred_element_type=f32)
            ).astype(b16)

        @pl.when(i == 0)
        def _():
            def far_away(k, inner):
                to = lax.rem(t + 1 + k, nt)

                @pl.when(jnp.logical_not(near(to)))
                def _():
                    give_ortho(to).start()

                return inner

            lax.fori_loop(0, nt - 1, far_away, 0)

        return carry

    lax.fori_loop(0, nt, ortho_of, 0)

    def drain(i, carry):
        d, e, c = moves(i)

        @pl.when(t < d)
        def _():
            to_right(rbuf.at[d, c], d, c).wait_send()

        @pl.when(t > e)
        def _():
            to_left(lbuf.at[e, c], e, c).wait_send()

        return carry

    lax.fori_loop(0, (nt - 1) * cuts, drain, 0)
    other.wait_send()

    def drain_pieces(i, carry):
        q = lax.rem(p + 1 + i, group)

        @pl.when(q < owners)
        def _():
            remote(part_of(q), pieces.at[p], p_send.at[q], p_recv.at[p], **at(q)).wait_send()

        @pl.when(p < owners)
        def _():
            remote(final_of(p), final_of(p), q_send.at[q], q_recv.at[p], **at(q)).wait_send()

        return carry

    lax.fori_loop(0, group - 1, drain_pieces, 0)

    def drain_gather(i, carry):
        q = lax.rem(t + 1 + i, nt)
        there = pl.ds(pl.multiple_of(q * share, share), share)

        @pl.when(near(q))
        def _():
            give_left(q).wait_send()

        @pl.when(jnp.logical_not(near(q)))
        def _():
            remote(ortho_ref.at[there], ortho_ref.at[there], ag_send.at[0], ag_recv.at[q], tp=q).wait_recv()
            give_ortho(q).wait_send()

        return carry

    lax.fori_loop(0, nt - 1, drain_gather, 0)


def mid(moment, grad, basis, nf, nt):
    _, rows, cols = moment.shape
    rank = basis.shape[2]
    share = rows // nt
    cuts = pick(share // 8, (4, 2, 1)) if share % 32 else 4
    sub = share // cuts
    half = rank // 2
    group = (nf // 2) * nt
    owners = min(group, half // 8)
    bits = pick(cols, (512, 256, 128))
    f32, b16 = jnp.float32, jnp.bfloat16
    dma = pltpu.SemaphoreType.DMA
    hbm = pl.BlockSpec(memory_space=pl.ANY)
    return pl.pallas_call(
        functools.partial(mid_kernel, nf, nt, cuts),
        out_shape=jax.ShapeDtypeStruct((rows, rank), b16),
        in_specs=[hbm, hbm, hbm],
        out_specs=pl.BlockSpec(memory_space=pltpu.VMEM),
        scratch_shapes=[
            pltpu.VMEM((rows, rank), f32),
            pltpu.VMEM((cols, rank), b16),
            pltpu.VMEM((cols, rank), b16),
            pltpu.VMEM((2, bits, rank), f32),
            pltpu.VMEM((2, share, cols), f32),
            pltpu.VMEM((2, share, cols), b16),
            dma((6,)),
            pltpu.VMEM((rows, rank), f32),
            pltpu.VMEM((nt, cuts, sub, rank), f32),
            pltpu.VMEM((nt, cuts, sub, rank), f32),
            pltpu.VMEM((rank, rank), f32),
            pltpu.VMEM((half, rank), f32),
            pltpu.VMEM((group, half // owners, rank), f32),
            pltpu.VMEM((rank, rank), f32),
            pltpu.VMEM((rank, rank), f32),
            pltpu.VMEM((rank, rank), f32),
            pltpu.VMEM((BLOCK, BLOCK), f32),
            pltpu.VMEM((BLOCK, BLOCK), f32),
            dma((2, nt, cuts)), dma((2, nt, cuts)),
            dma((2,)), dma((2,)),
            dma((group,)), dma((group,)),
            dma((group,)), dma((group,)),
            dma((nt,)), dma((nt,)),
        ],
        compiler_params=pltpu.CompilerParams(
            vmem_limit_bytes=56 << 20, collective_id=0, has_side_effects=True
        ),
        cost_estimate=pl.CostEstimate(
            flops=60_000_000_000, bytes_accessed=8 * rows * cols, transcendentals=0
        ),
        name="mid",
    )(moment, grad, basis)


def right_kernel(
    nf, nt, cuts, cols, part_ref, ortho_ref, right_ref, inv_ref, far_ortho, far_right, far_inv,
    mbuf, sbuf, ybuf, sqs,
    m_send, m_recv, y_send, y_recv, g_send, g_recv, w_send, w_recv, sq_send, sq_recv,
    x_send, x_recv, o_send, o_recv,
):
    f, t = lax.axis_index("fsdp"), lax.axis_index("tp")
    core = lax.rem(f, 2)
    y = f // 2
    ny = nf // 2
    mate = f + 1 - 2 * core
    half = part_ref.shape[0] // 2
    quarter = half // ny
    sub = quarter // cuts
    n = nf * nt
    me = f * nt + t
    f32, b16 = jnp.float32, jnp.bfloat16

    far = 1 - lax.axis_index("rollout")
    share = far_ortho.shape[0] // nt

    greet(nf, nt, True)

    def across(src, dst, i):
        return remote(src, dst, x_send.at[i], x_recv.at[i], rollout=far)

    def block(q):
        return pl.ds(pl.multiple_of(q * share, share), share)

    cross_ortho = across(ortho_ref.at[block(t)], far_ortho.at[block(t)], cuts)
    cross_ortho.start()

    def along(q, source):
        rows = block(source)
        return remote(far_ortho.at[rows], far_ortho.at[rows], o_send.at[q], o_recv.at[source], tp=q)

    def rows_of(h, q, c):
        return pl.ds(pl.multiple_of(h * half + q * quarter + c * sub, sub), sub)

    def order(i):
        return lax.rem(y + 1 + i // cuts, ny), lax.rem(i, cuts)

    def to_mate(q, c):
        return remote(
            part_ref.at[rows_of(1 - core, q, c)], mbuf.at[q, c], m_send.at[q, c], m_recv.at[q, c],
            fsdp=mate,
        )

    def start_mate(i, carry):
        q, c = order(i)
        to_mate(q, c).start()
        return carry

    lax.fori_loop(0, ny * cuts, start_mate, 0)

    def to_peer(q, c):
        return remote(
            sbuf.at[q, c], ybuf.at[y, c], y_send.at[q, c], y_recv.at[y, c], fsdp=2 * q + core
        )

    def pair_sum(i, carry):
        q, c = order(i)
        to_mate(q, c).wait_recv()
        sbuf[q, c] = (part_ref[rows_of(core, q, c), :].astype(f32) + mbuf[q, c].astype(f32)).astype(b16)
        to_peer(q, c).start()
        return carry

    lax.fori_loop(0, (ny - 1) * cuts, pair_sum, 0)

    def spread(q, c):
        rows = rows_of(core, y, c)
        return remote(
            right_ref.at[rows], right_ref.at[rows], g_send.at[q, c], g_recv.at[y, c], fsdp=2 * q + core
        )

    def cross_right(c):
        return across(
            right_ref.at[rows_of(core, y, c)], far_right.at[pl.ds(pl.multiple_of(c * sub, sub), sub)], c
        )

    def to_other_core(q, c):
        rows = rows_of(core, q, c)
        return remote(
            right_ref.at[rows], right_ref.at[rows], w_send.at[q, c], w_recv.at[q, c], fsdp=mate
        )

    sqs[me] = jnp.zeros_like(sqs[me])

    def reduce(c, carry):
        to_mate(y, c).wait_recv()
        total = part_ref[rows_of(core, y, c), :].astype(f32) + mbuf[y, c].astype(f32)

        def add(i, acc):
            q = lax.rem(y + 1 + i, ny)
            remote(
                sbuf.at[y, c], ybuf.at[q, c], y_send.at[q, c], y_recv.at[q, c], fsdp=2 * q + core
            ).wait_recv()
            return acc + ybuf[q, c].astype(f32)

        total = lax.fori_loop(0, ny - 1, add, total)
        rows = rows_of(core, y, c)
        right_ref[rows, :] = total.astype(b16)
        sqs[me] = sqs[me] + jnp.sum((total * total).reshape(sub // 8, 8, total.shape[1]), axis=0)

        cross_right(c).start()
        to_other_core(y, c).start()
        return carry

    lax.fori_loop(0, cuts, reduce, 0)

    def to_all(q):
        return remote(
            sqs.at[me], sqs.at[me], sq_send.at[q], sq_recv.at[me], fsdp=q // nt, tp=lax.rem(q, nt)
        )

    def start_squares(i, carry):
        to_all(lax.rem(me + 1 + i, n)).start()
        return carry

    lax.fori_loop(0, n - 1, start_squares, 0)

    def start_spread(i, carry):
        spread(*order(i)).start()
        return carry

    lax.fori_loop(0, (ny - 1) * cuts, start_spread, 0)
    cross_ortho.wait_recv()

    def start_along(i, carry):
        along(lax.rem(t + 1 + i, nt), t).start()
        return carry

    lax.fori_loop(0, nt - 1, start_along, 0)

    def forward(i, carry):
        q, c = order(i)
        rows = rows_of(core, q, c)
        remote(
            right_ref.at[rows], right_ref.at[rows], g_send.at[q, c], g_recv.at[q, c], fsdp=2 * q + core
        ).wait_recv()
        to_other_core(q, c).start()
        return carry

    lax.fori_loop(0, (ny - 1) * cuts, forward, 0)

    def got_square(i, carry):
        q = lax.rem(me + 1 + i, n)
        remote(
            sqs.at[q], sqs.at[q], sq_send.at[q], sq_recv.at[q], fsdp=q // nt, tp=lax.rem(q, nt)
        ).wait_recv()
        return carry

    lax.fori_loop(0, n - 1, got_square, 0)
    total = lax.fori_loop(1, n, lambda q, acc: acc + sqs[q], sqs[0])
    meansq = jnp.sum(total, axis=0, keepdims=True) / cols
    inv_ref[...] = jnp.broadcast_to(lax.rsqrt(meansq + 1e-06), inv_ref.shape)
    cross_inv = across(inv_ref, far_inv, cuts + 1)
    cross_inv.start()

    def finish(i, carry):
        q, c = order(i)
        rows = rows_of(1 - core, q, c)
        remote(
            right_ref.at[rows], right_ref.at[rows], w_send.at[q, c], w_recv.at[q, c], fsdp=mate
        ).wait_recv()
        to_mate(q, c).wait_send()
        to_other_core(q, c).wait_send()

        @pl.when(q != y)
        def _():
            to_peer(q, c).wait_send()
            spread(q, c).wait_send()

        return carry

    lax.fori_loop(0, ny * cuts, finish, 0)

    def drain_squares(i, carry):
        to_all(lax.rem(me + 1 + i, n)).wait_send()
        return carry

    lax.fori_loop(0, n - 1, drain_squares, 0)

    def finish_cross(c, carry):
        cross_right(c).wait()
        return carry

    lax.fori_loop(0, cuts, finish_cross, 0)
    cross_ortho.wait_send()
    cross_inv.wait()

    def finish_along(i, carry):
        q = lax.rem(t + 1 + i, nt)
        along(q, q).wait_recv()
        along(q, t).wait_send()
        return carry

    lax.fori_loop(0, nt - 1, finish_along, 0)


def sub_blocks(quarter):
    for cuts in (4, 2):
        if quarter % (16 * cuts) == 0:
            return cuts
    return 1


def right_sum(part, ortho, nf, nt, cols):
    mine, rank = part.shape
    ny = nf // 2
    quarter = mine // nf
    cuts = sub_blocks(quarter)
    sub = quarter // cuts
    n = nf * nt
    b16, f32 = jnp.bfloat16, jnp.float32
    dma = pltpu.SemaphoreType.DMA
    vmem = pl.BlockSpec(memory_space=pltpu.VMEM)
    return pl.pallas_call(
        functools.partial(right_kernel, nf, nt, cuts, cols),
        out_shape=(
            jax.ShapeDtypeStruct((mine, rank), b16),
            jax.ShapeDtypeStruct((8, rank), f32),
            jax.ShapeDtypeStruct(ortho.shape, b16),
            jax.ShapeDtypeStruct((quarter, rank), b16),
            jax.ShapeDtypeStruct((8, rank), f32),
        ),
        in_specs=[vmem, vmem],
        out_specs=(vmem,) * 5,
        scratch_shapes=[
            pltpu.VMEM((ny, cuts, sub, rank), b16),
            pltpu.VMEM((ny, cuts, sub, rank), b16),
            pltpu.VMEM((ny, cuts, sub, rank), b16),
            pltpu.VMEM((n, 8, rank), f32),
            dma((ny, cuts)), dma((ny, cuts)),
            dma((ny, cuts)), dma((ny, cuts)),
            dma((ny, cuts)), dma((ny, cuts)),
            dma((ny, cuts)), dma((ny, cuts)),
            dma((n,)), dma((n,)),
            dma((cuts + 2,)), dma((cuts + 2,)),
            dma((nt,)), dma((nt,)),
        ],
        compiler_params=pltpu.CompilerParams(
            vmem_limit_bytes=40 << 20, collective_id=1, has_side_effects=True
        ),
        cost_estimate=pl.CostEstimate(
            flops=10_000_000_000, bytes_accessed=4 * mine * rank, transcendentals=0
        ),
        name="right_sum",
    )(part, ortho)


def own_kernel(
    who_ref, w_ref, g_ref, m_ref, ortho_ref, right_ref, inv_ref, new_ref, both_ref, moment_ref, basis_ref
):
    f32 = jnp.float32
    dims = (((1,), (1,)), ((), ()))
    tc = w_ref.shape[2]
    right = right_ref[pl.ds(pl.multiple_of(pl.program_id(0) * tc, tc), tc), :]
    ortho = ortho_ref[...]
    basis = right.astype(f32) * inv_ref[0:1, :]
    basis_ref[0] = basis
    update = lax.dot_general(ortho, basis.astype(jnp.bfloat16), dims, preferred_element_type=f32)
    value = (w_ref[0].astype(f32) - 0.3 * update).astype(jnp.bfloat16)
    new_ref[0] = value
    both_ref[0] = value
    blend = m_ref[0] + g_ref[0].astype(f32)
    moment_ref[0] = blend - 0.05 * lax.dot_general(ortho, right, dims, preferred_element_type=f32)


def apply_own(who, w, g, m, ortho, right, inv):
    _, rows, cols = w.shape
    rank = ortho.shape[1]
    tc = pick(cols, (512, 256, 128))
    spec = pl.BlockSpec((1, rows, tc), lambda j, who: (0, 0, j))
    f32, b16 = jnp.float32, jnp.bfloat16
    return pl.pallas_call(
        own_kernel,
        out_shape=(
            jax.ShapeDtypeStruct((1, rows, cols), b16),
            jax.ShapeDtypeStruct((2, rows, cols), b16),
            jax.ShapeDtypeStruct((1, rows, cols), f32),
            jax.ShapeDtypeStruct((1, cols, rank), f32),
        ),
        grid_spec=pltpu.PrefetchScalarGridSpec(
            num_scalar_prefetch=1,
            grid=(cols // tc,),
            in_specs=[
                spec,
                spec,
                spec,
                pl.BlockSpec(memory_space=pltpu.VMEM),
                pl.BlockSpec(memory_space=pltpu.VMEM),
                pl.BlockSpec(memory_space=pltpu.VMEM),
            ],
            out_specs=(
                spec,
                pl.BlockSpec((1, rows, tc), lambda j, who: (who[0], 0, j)),
                spec,
                pl.BlockSpec((1, tc, rank), lambda j, who: (0, j, 0)),
            ),
        ),
        compiler_params=pltpu.CompilerParams(vmem_limit_bytes=48 << 20),
        cost_estimate=pl.CostEstimate(
            flops=30_000_000_000, bytes_accessed=18 * rows * cols, transcendentals=0
        ),
        name="apply_own",
    )(who, w, g, m, ortho, right, inv)


def other_kernel(nf, who_ref, *refs):
    rights = refs[:nf]
    ortho, w_ref, inv_ref, _, both_ref, base = refs[nf:]
    quarter = rights[0].shape[0]
    f32, b16 = jnp.float32, jnp.bfloat16
    j = pl.program_id(0)

    @pl.when(j == 0)
    def _():
        inv = inv_ref[0:1, :]
        for k, piece in enumerate(rights):
            place = pl.ds(pl.multiple_of(who_ref[1 + k] * quarter, quarter), quarter)
            base[place, :] = (piece[...].astype(f32) * inv).astype(b16)

    tc = w_ref.shape[2]
    update = lax.dot_general(
        ortho[...],
        base[pl.ds(pl.multiple_of(j * tc, tc), tc), :],
        (((1,), (1,)), ((), ())),
        preferred_element_type=f32,
    )
    both_ref[0] = (w_ref[0].astype(f32) - 0.3 * update).astype(b16)


def apply_other(who, rights, ortho, w, inv, both):
    _, rows, cols = w.shape
    rank = inv.shape[1]
    nf = len(rights)
    tc = pick(cols, (512, 256, 128))
    whole = pl.BlockSpec(memory_space=pltpu.VMEM)
    return pl.pallas_call(
        functools.partial(other_kernel, nf),
        out_shape=jax.ShapeDtypeStruct((2, rows, cols), jnp.bfloat16),
        grid_spec=pltpu.PrefetchScalarGridSpec(
            num_scalar_prefetch=1,
            grid=(cols // tc,),
            in_specs=[whole] * (nf + 1)
            + [
                pl.BlockSpec((1, rows, tc), lambda j, who: (0, 0, j)),
                whole,
                pl.BlockSpec(memory_space=pl.ANY),
            ],
            out_specs=pl.BlockSpec((1, rows, tc), lambda j, who: (who[0], 0, j)),
            scratch_shapes=[pltpu.VMEM((cols, rank), jnp.bfloat16)],
        ),
        input_output_aliases={nf + 4: 0},
        compiler_params=pltpu.CompilerParams(vmem_limit_bytes=40 << 20),
        cost_estimate=pl.CostEstimate(
            flops=2 * rows * cols * rank, bytes_accessed=4 * rows * cols, transcendentals=0
        ),
        name="apply_other",
    )(who, *rights, ortho, w, inv, both)


def body(weights, gradient, momentum, basis):
    swap = functools.partial(lax.ppermute, axis_name="rollout", perm=[(0, 1), (1, 0)])
    me = lax.axis_index("rollout")
    f = lax.axis_index("fsdp")
    nf, nt = lax.axis_size("fsdp"), lax.axis_size("tp")
    cols = weights.shape[2] * nt
    weights_other = swap(weights)
    blend = momentum[0] + gradient[0].astype(jnp.float32)
    ortho = mid(momentum, gradient, basis, nf, nt)
    partial_right = lax.dot_general(
        blend.astype(jnp.bfloat16),
        ortho,
        (((0,), (0,)), ((), ())),
        preferred_element_type=jnp.float32,
    ).astype(jnp.bfloat16)
    right, inv, far_ortho, far_right, inv_other = right_sum(partial_right, ortho, nf, nt, cols)
    ny = nf // 2
    core, y = f % 2, f // 2
    mates = [(i, i ^ 1) for i in range(nf)]
    rights, right_places = [far_right], [core * ny + y]
    for k in range(1, ny):
        rights.append(
            lax.ppermute(far_right, "fsdp", [(i, ((i // 2 - k) % ny) * 2 + i % 2) for i in range(nf)])
        )
        right_places.append(core * ny + (y + k) % ny)
    for k in range(ny):
        rights.append(lax.ppermute(rights[k], "fsdp", mates))
        right_places.append((1 - core) * ny + (y + k) % ny)
    weight_new, both, moment_new, basis_new = apply_own(
        me.reshape(1), weights, gradient, momentum, ortho, right, inv
    )
    who = jnp.stack([1 - me] + right_places).astype(jnp.int32)
    both = apply_other(who, rights, far_ortho, weights_other, inv_other, both)
    return (weight_new, moment_new, basis_new, both)


def solution(mesh):
    return jax.shard_map(
        body,
        mesh=mesh,
        in_specs=(
            P("rollout", "fsdp", "tp"),
            P("rollout", "fsdp", "tp"),
            P("rollout", "fsdp", "tp"),
            P("rollout", "tp", None),
        ),
        out_specs=(
            P("rollout", "fsdp", "tp"),
            P("rollout", "fsdp", "tp"),
            P("rollout", "tp", None),
            P(None, "fsdp", "tp"),
        ),
        check_vma=False,
    )
```

```python
import functools

import jax
import jax.numpy as jnp
from jax import lax
from jax.experimental import pallas as pl
from jax.experimental.pallas import tpu as pltpu
from jax.sharding import PartitionSpec as P


HIGH = lax.Precision.HIGHEST
BLOCK = 128
STRIP = 32
MESH = pl.DeviceIdType.MESH


def dot_t(a, b):
    return lax.dot_general(
        a, b, (((1,), (1,)), ((), ())), precision=HIGH, preferred_element_type=jnp.float32
    )


def pick(n, sizes):
    for s in sizes:
        if n % s == 0:
            return s
    return n


def remote(src, dst, send, recv, **where):
    return pltpu.make_async_remote_copy(
        src_ref=src, dst_ref=dst, send_sem=send, recv_sem=recv, device_id=where, device_id_type=MESH
    )


def greet(nf, nt, across=False):
    f, t = lax.axis_index("fsdp"), lax.axis_index("tp")
    barrier = pltpu.get_barrier_semaphore()
    n = nf * nt
    me = f * nt + t

    def one(i, carry):
        q = lax.rem(me + 1 + i, n)
        pl.semaphore_signal(
            barrier, inc=1, device_id={"fsdp": q // nt, "tp": lax.rem(q, nt)}, device_id_type=MESH
        )
        return carry

    lax.fori_loop(0, n - 1, one, 0)
    if across:
        pl.semaphore_signal(
            barrier, inc=1, device_id={"rollout": 1 - lax.axis_index("rollout")}, device_id_type=MESH
        )
    pl.semaphore_wait(barrier, n - 1 + across)


def factor_block(s_ref, v_ref):
    nb = BLOCK
    tile = STRIP
    lane = lax.broadcasted_iota(jnp.int32, (tile, nb), 1)
    sub = lax.broadcasted_iota(jnp.int32, (tile, nb), 0)

    def strip(j, carry):
        rows = pl.ds(pl.multiple_of(j * tile, tile), tile)
        s = s_ref[rows, :]
        v = v_ref[rows, :]
        turned = pltpu.roll(s, lax.rem(nb - j * tile, nb), 1)
        cols = [jnp.broadcast_to(turned[:, i : i + 1], (tile, nb)) for i in range(tile)]
        pivot = jnp.ones((tile, nb), jnp.float32)
        recip = jnp.ones((tile, nb), jnp.float32)
        for i in range(tile):
            p = jnp.broadcast_to(cols[i][i : i + 1, :], (tile, nb))
            rp = 1.0 / p
            pivot = jnp.where(sub == i, p, pivot)
            recip = jnp.where(sub == i, rp, recip)
            if i < tile - 1:
                by = jnp.where(sub > i, cols[i] * rp, 0.0)
                for m in range(i + 1, tile):
                    cols[m] = cols[m] - by * jnp.broadcast_to(cols[m][i : i + 1, :], (tile, nb))
                s = s - by * jnp.broadcast_to(s[i : i + 1, :], (tile, nb))
                v = v - by * jnp.broadcast_to(v[i : i + 1, :], (tile, nb))
        below = jnp.where(lane >= (j + 1) * tile, s * recip, 0.0)
        change = lax.dot_general(
            below,
            jnp.concatenate([s, v], axis=1),
            (((0,), (0,)), ((), ())),
            precision=HIGH,
            preferred_element_type=jnp.float32,
        )
        s_ref[...] = s_ref[...] - change[:, :nb]
        v_ref[...] = v_ref[...] - change[:, nb:]
        r = lax.rsqrt(pivot)
        r = r * (1.5 - 0.5 * pivot * r * r)
        v_ref[rows, :] = v * r
        return carry

    lax.fori_loop(0, nb // tile, strip, 0)


def factor(a_ref, x_ref, w_ref, s_ref, v_ref):
    n = a_ref.shape[0]
    nb = BLOCK
    w_ref[...] = jnp.where(
        lax.broadcasted_iota(jnp.int32, (n, n), 0) == lax.broadcasted_iota(jnp.int32, (n, n), 1),
        1.0,
        0.0,
    ).astype(jnp.float32)
    lane = lax.broadcasted_iota(jnp.int32, (nb, nb), 1)
    sub = lax.broadcasted_iota(jnp.int32, (nb, nb), 0)

    for lo in range(0, n, nb):
        hi = lo + nb
        s_ref[...] = a_ref[lo:hi, lo:hi]
        v_ref[...] = jnp.where(lane == sub, 1.0, 0.0).astype(jnp.float32)
        factor_block(s_ref, v_ref)
        inv = v_ref[...]
        x = jnp.dot(inv, w_ref[lo:hi, :hi], precision=HIGH, preferred_element_type=jnp.float32)
        x_ref[lo:hi, :hi] = x
        if hi < n:
            x_ref[lo:hi, hi:] = jnp.zeros((nb, n - hi), jnp.float32)
            panel = dot_t(a_ref[hi:, lo:hi], inv)
            a_ref[hi:, hi:] = a_ref[hi:, hi:] - dot_t(panel, panel)
            w_ref[hi:, :hi] = w_ref[hi:, :hi] - jnp.dot(
                panel, x, precision=HIGH, preferred_element_type=jnp.float32
            )


def mid_kernel(
    nf, nt, cuts, moment_ref, grad_ref, basis_ref, ortho_ref, blend_ref,
    part_ref, high, low, basis_stage, moment_stage, grad_stage, in_sem, left, rbuf, lbuf, gpart, gmate, pieces, gram, inverse, work, s_ref, v_ref,
    rs_send, rs_recv, mate_send, mate_recv, p_send, p_recv, q_send, q_recv, ag_send, ag_recv,
):
    f, t = lax.axis_index("fsdp"), lax.axis_index("tp")
    core = lax.rem(f, 2)
    mate = f + 1 - 2 * core
    rows, rank = part_ref.shape
    share = rows // nt
    sub = share // cuts
    half = rank // 2
    bits = basis_stage.shape[1]
    pieces_of_basis = high.shape[0] // bits
    f32, b16 = jnp.float32, jnp.bfloat16

    def block_at(i):
        k = jnp.where(lax.rem(i, 2) == 0, nt - 1 - i // 2, i // 2)
        return jnp.where(t < (nt + 1) // 2, k, nt - 1 - k)

    def fetch_rows(i):
        where = pl.ds(pl.multiple_of(block_at(i) * share, share), share)
        slot = lax.rem(i, 2)
        return (
            pltpu.make_async_copy(moment_ref.at[0, where], moment_stage.at[slot], in_sem.at[slot]),
            pltpu.make_async_copy(grad_ref.at[0, where], grad_stage.at[slot], in_sem.at[2 + slot]),
        )

    def fetch_basis(i):
        where = pl.ds(pl.multiple_of(i * bits, bits), bits)
        slot = lax.rem(i, 2)
        return pltpu.make_async_copy(basis_ref.at[0, where], basis_stage.at[slot], in_sem.at[4 + slot])

    fetch_basis(0).start()
    for copy in fetch_rows(0):
        copy.start()
    group = (nf // 2) * nt
    owners = min(group, half // 8)
    piece = half // owners
    p = (f // 2) * nt + t

    greet(nf, nt)

    def chunk(d, c):
        return part_ref.at[pl.ds(pl.multiple_of(d * share + c * sub, sub), sub)]

    def moves(i):
        c = lax.rem(i, cuts)
        k = i // cuts
        return nt - 1 - k, k, c

    def to_right(src, d, c):
        return remote(src, rbuf.at[d, c], rs_send.at[0, d, c], rs_recv.at[0, d, c], tp=t + 1)

    def to_left(src, e, c):
        return remote(src, lbuf.at[e, c], rs_send.at[1, e, c], rs_recv.at[1, e, c], tp=t - 1)

    def split_basis(i, carry):
        fetch_basis(i).wait()

        @pl.when(i + 1 < pieces_of_basis)
        def _():
            fetch_basis(i + 1).start()

        value = basis_stage[lax.rem(i, 2)]
        where = pl.ds(pl.multiple_of(i * bits, bits), bits)
        top = value.astype(b16)
        high[where, :] = top
        low[where, :] = (value - top.astype(f32)).astype(b16)
        return carry

    lax.fori_loop(0, pieces_of_basis, split_basis, 0)

    def left_block(i, carry):
        slot = lax.rem(i, 2)
        for copy in fetch_rows(i):
            copy.wait()

        @pl.when(i + 1 < nt)
        def _():
            for copy in fetch_rows(i + 1):
                copy.start()

        d = block_at(i)
        value = moment_stage[slot] + grad_stage[slot].astype(f32)
        top = value.astype(b16)
        rest = (value - top.astype(f32)).astype(b16)
        blend_ref[pl.ds(pl.multiple_of(d * share, share), share), :] = top
        part_ref[pl.ds(pl.multiple_of(d * share, share), share), :] = (
            jnp.dot(top, low[...], preferred_element_type=f32)
            + jnp.dot(rest, high[...], preferred_element_type=f32)
            + jnp.dot(top, high[...], preferred_element_type=f32)
        )

        def begin(c, inner):
            @pl.when(jnp.logical_and(t == 0, d > 0))
            def _():
                to_right(chunk(d, c), d, c).start()

            @pl.when(jnp.logical_and(t == nt - 1, d < nt - 1))
            def _():
                to_left(chunk(d, c), d, c).start()

            return inner

        lax.fori_loop(0, cuts, begin, 0)
        return carry

    lax.fori_loop(0, nt, left_block, 0)

    def scatter(i, carry):
        d, e, c = moves(i)

        @pl.when(jnp.logical_and(t < d, t > 0))
        def _():
            to_right(rbuf.at[d, c], d, c).wait_recv()
            rbuf[d, c] = rbuf[d, c] + chunk(d, c)[...]
            to_right(rbuf.at[d, c], d, c).start()

        @pl.when(jnp.logical_and(t > e, t < nt - 1))
        def _():
            to_left(lbuf.at[e, c], e, c).wait_recv()
            lbuf[e, c] = lbuf[e, c] + chunk(e, c)[...]
            to_left(lbuf.at[e, c], e, c).start()

        return carry

    lax.fori_loop(0, (nt - 1) * cuts, scatter, 0)

    def mine(c, carry):
        here = pl.ds(pl.multiple_of(t * share + c * sub, sub), sub)
        left[here, :] = part_ref[here, :]

        @pl.when(t > 0)
        def _():
            to_right(rbuf.at[t, c], t, c).wait_recv()
            left[here, :] = left[here, :] + rbuf[t, c]

        @pl.when(t < nt - 1)
        def _():
            to_left(lbuf.at[t, c], t, c).wait_recv()
            left[here, :] = left[here, :] + lbuf[t, c]

        return carry

    lax.fori_loop(0, cuts, mine, 0)

    here = pl.ds(pl.multiple_of(t * share, share), share)
    own = left[here, :]
    gpart[...] = lax.dot_general(
        own, own, (((0,), (0,)), ((), ())), precision=HIGH, preferred_element_type=jnp.float32
    )
    keep = pl.ds(pl.multiple_of(core * half, half), half)
    give = pl.ds(pl.multiple_of((1 - core) * half, half), half)
    pair = remote(gpart.at[give], gmate, mate_send.at[0], mate_recv.at[0], fsdp=mate)
    pair.start()
    pair.wait_recv()
    gmate[...] = gmate[...] + gpart[keep, :]

    def at(q):
        return {"fsdp": 2 * (q // nt) + core, "tp": lax.rem(q, nt)}

    def part_of(q):
        return gmate.at[pl.ds(pl.multiple_of(q * piece, piece), piece)]

    def send_piece(i, carry):
        q = lax.rem(p + 1 + i, group)

        @pl.when(q < owners)
        def _():
            remote(part_of(q), pieces.at[p], p_send.at[q], p_recv.at[p], **at(q)).start()

        return carry

    lax.fori_loop(0, group - 1, send_piece, 0)

    def final_of(q):
        return gram.at[pl.ds(pl.multiple_of(core * half + q * piece, piece), piece)]

    @pl.when(p < owners)
    def _():
        pieces[p] = part_of(p)[...]

        def got(i, carry):
            q = lax.rem(p + 1 + i, group)
            remote(part_of(p), pieces.at[q], p_send.at[0], p_recv.at[q], **at(q)).wait_recv()
            return carry

        lax.fori_loop(0, group - 1, got, 0)
        final_of(p)[...] = lax.fori_loop(
            1, group, lambda q, acc: acc + pieces[q], pieces[0]
        )

        def spread(i, carry):
            q = lax.rem(p + 1 + i, group)
            remote(final_of(p), final_of(p), q_send.at[q], q_recv.at[p], **at(q)).start()
            return carry

        lax.fori_loop(0, group - 1, spread, 0)

    def got_final(q, carry):
        @pl.when(q != p)
        def _():
            remote(final_of(q), final_of(q), q_send.at[0], q_recv.at[q], **at(q)).wait_recv()

        return carry

    lax.fori_loop(0, owners, got_final, 0)
    other = remote(gram.at[keep], gram.at[keep], mate_send.at[1], mate_recv.at[1], fsdp=mate)
    other.start()

    def near(q):
        return jnp.logical_or(q == t + 1, q == t - 1)

    def give_left(q):
        return remote(left.at[here], left.at[here], ag_send.at[q], ag_recv.at[t], tp=q)

    def give_ortho(q):
        return remote(ortho_ref.at[here], ortho_ref.at[here], ag_send.at[q], ag_recv.at[t], tp=q)

    def gather(i, carry):
        q = lax.rem(t + 1 + i, nt)

        @pl.when(near(q))
        def _():
            give_left(q).start()

        return carry

    lax.fori_loop(0, nt - 1, gather, 0)
    remote(gram.at[give], gram.at[give], mate_send.at[1], mate_recv.at[1], fsdp=mate).wait_recv()
    pair.wait_send()
    gpart[...] = gram[...]
    factor(gpart, inverse, work, s_ref, v_ref)

    inv_high = inverse[...].astype(b16)
    inv_low = (inverse[...] - inv_high.astype(f32)).astype(b16)

    def ortho_of(i, carry):
        q = lax.rem(t + i, nt)
        there = pl.ds(pl.multiple_of(q * share, share), share)

        @pl.when(near(q))
        def _():
            remote(left.at[there], left.at[there], ag_send.at[0], ag_recv.at[q], tp=q).wait_recv()

        @pl.when(jnp.logical_or(i == 0, near(q)))
        def _():
            value = left[there, :]
            top = value.astype(b16)
            rest = (value - top.astype(f32)).astype(b16)
            dims = (((1,), (1,)), ((), ()))
            ortho_ref[there, :] = (
                lax.dot_general(top, inv_low, dims, preferred_element_type=f32)
                + lax.dot_general(rest, inv_high, dims, preferred_element_type=f32)
                + lax.dot_general(top, inv_high, dims, preferred_element_type=f32)
            ).astype(b16)

        @pl.when(i == 0)
        def _():
            def far_away(k, inner):
                to = lax.rem(t + 1 + k, nt)

                @pl.when(jnp.logical_not(near(to)))
                def _():
                    give_ortho(to).start()

                return inner

            lax.fori_loop(0, nt - 1, far_away, 0)

        return carry

    lax.fori_loop(0, nt, ortho_of, 0)

    def drain(i, carry):
        d, e, c = moves(i)

        @pl.when(t < d)
        def _():
            to_right(rbuf.at[d, c], d, c).wait_send()

        @pl.when(t > e)
        def _():
            to_left(lbuf.at[e, c], e, c).wait_send()

        return carry

    lax.fori_loop(0, (nt - 1) * cuts, drain, 0)
    other.wait_send()

    def drain_pieces(i, carry):
        q = lax.rem(p + 1 + i, group)

        @pl.when(q < owners)
        def _():
            remote(part_of(q), pieces.at[p], p_send.at[q], p_recv.at[p], **at(q)).wait_send()

        @pl.when(p < owners)
        def _():
            remote(final_of(p), final_of(p), q_send.at[q], q_recv.at[p], **at(q)).wait_send()

        return carry

    lax.fori_loop(0, group - 1, drain_pieces, 0)

    def drain_gather(i, carry):
        q = lax.rem(t + 1 + i, nt)
        there = pl.ds(pl.multiple_of(q * share, share), share)

        @pl.when(near(q))
        def _():
            give_left(q).wait_send()

        @pl.when(jnp.logical_not(near(q)))
        def _():
            remote(ortho_ref.at[there], ortho_ref.at[there], ag_send.at[0], ag_recv.at[q], tp=q).wait_recv()
            give_ortho(q).wait_send()

        return carry

    lax.fori_loop(0, nt - 1, drain_gather, 0)


def mid(moment, grad, basis, nf, nt):
    _, rows, cols = moment.shape
    rank = basis.shape[2]
    share = rows // nt
    cuts = pick(share // 8, (4, 2, 1)) if share % 32 else 4
    sub = share // cuts
    half = rank // 2
    group = (nf // 2) * nt
    owners = min(group, half // 8)
    bits = pick(cols, (512, 256, 128))
    f32, b16 = jnp.float32, jnp.bfloat16
    dma = pltpu.SemaphoreType.DMA
    hbm = pl.BlockSpec(memory_space=pl.ANY)
    return pl.pallas_call(
        functools.partial(mid_kernel, nf, nt, cuts),
        out_shape=(
            jax.ShapeDtypeStruct((rows, rank), b16),
            jax.ShapeDtypeStruct((rows, cols), b16),
        ),
        in_specs=[hbm, hbm, hbm],
        out_specs=(pl.BlockSpec(memory_space=pltpu.VMEM),) * 2,
        scratch_shapes=[
            pltpu.VMEM((rows, rank), f32),
            pltpu.VMEM((cols, rank), b16),
            pltpu.VMEM((cols, rank), b16),
            pltpu.VMEM((2, bits, rank), f32),
            pltpu.VMEM((2, share, cols), f32),
            pltpu.VMEM((2, share, cols), b16),
            dma((6,)),
            pltpu.VMEM((rows, rank), f32),
            pltpu.VMEM((nt, cuts, sub, rank), f32),
            pltpu.VMEM((nt, cuts, sub, rank), f32),
            pltpu.VMEM((rank, rank), f32),
            pltpu.VMEM((half, rank), f32),
            pltpu.VMEM((group, half // owners, rank), f32),
            pltpu.VMEM((rank, rank), f32),
            pltpu.VMEM((rank, rank), f32),
            pltpu.VMEM((rank, rank), f32),
            pltpu.VMEM((BLOCK, BLOCK), f32),
            pltpu.VMEM((BLOCK, BLOCK), f32),
            dma((2, nt, cuts)), dma((2, nt, cuts)),
            dma((2,)), dma((2,)),
            dma((group,)), dma((group,)),
            dma((group,)), dma((group,)),
            dma((nt,)), dma((nt,)),
        ],
        compiler_params=pltpu.CompilerParams(
            vmem_limit_bytes=52 << 20, collective_id=0, has_side_effects=True
        ),
        cost_estimate=pl.CostEstimate(
            flops=60_000_000_000, bytes_accessed=8 * rows * cols, transcendentals=0
        ),
        name="mid",
    )(moment, grad, basis)


def right_kernel(
    nf, nt, cuts, cols, part_ref, ortho_ref, right_ref, inv_ref, far_ortho, far_right, far_inv,
    mbuf, sbuf, ybuf, sqs,
    m_send, m_recv, y_send, y_recv, g_send, g_recv, w_send, w_recv, sq_send, sq_recv,
    x_send, x_recv, o_send, o_recv,
):
    f, t = lax.axis_index("fsdp"), lax.axis_index("tp")
    core = lax.rem(f, 2)
    y = f // 2
    ny = nf // 2
    mate = f + 1 - 2 * core
    half = part_ref.shape[0] // 2
    quarter = half // ny
    sub = quarter // cuts
    n = nf * nt
    me = f * nt + t
    f32, b16 = jnp.float32, jnp.bfloat16

    far = 1 - lax.axis_index("rollout")
    share = far_ortho.shape[0] // nt

    greet(nf, nt, True)

    def across(src, dst, i):
        return remote(src, dst, x_send.at[i], x_recv.at[i], rollout=far)

    def block(q):
        return pl.ds(pl.multiple_of(q * share, share), share)

    cross_ortho = across(ortho_ref.at[block(t)], far_ortho.at[block(t)], cuts)
    cross_ortho.start()

    def along(q, source):
        rows = block(source)
        return remote(far_ortho.at[rows], far_ortho.at[rows], o_send.at[q], o_recv.at[source], tp=q)

    def rows_of(h, q, c):
        return pl.ds(pl.multiple_of(h * half + q * quarter + c * sub, sub), sub)

    def order(i):
        return lax.rem(y + 1 + i // cuts, ny), lax.rem(i, cuts)

    def to_mate(q, c):
        return remote(
            part_ref.at[rows_of(1 - core, q, c)], mbuf.at[q, c], m_send.at[q, c], m_recv.at[q, c],
            fsdp=mate,
        )

    def start_mate(i, carry):
        q, c = order(i)
        to_mate(q, c).start()
        return carry

    lax.fori_loop(0, ny * cuts, start_mate, 0)

    def to_peer(q, c):
        return remote(
            sbuf.at[q, c], ybuf.at[y, c], y_send.at[q, c], y_recv.at[y, c], fsdp=2 * q + core
        )

    def pair_sum(i, carry):
        q, c = order(i)
        to_mate(q, c).wait_recv()
        sbuf[q, c] = (part_ref[rows_of(core, q, c), :].astype(f32) + mbuf[q, c].astype(f32)).astype(b16)
        to_peer(q, c).start()
        return carry

    lax.fori_loop(0, (ny - 1) * cuts, pair_sum, 0)

    def spread(q, c):
        rows = rows_of(core, y, c)
        return remote(
            right_ref.at[rows], right_ref.at[rows], g_send.at[q, c], g_recv.at[y, c], fsdp=2 * q + core
        )

    def cross_right(c):
        return across(
            right_ref.at[rows_of(core, y, c)], far_right.at[pl.ds(pl.multiple_of(c * sub, sub), sub)], c
        )

    def to_other_core(q, c):
        rows = rows_of(core, q, c)
        return remote(
            right_ref.at[rows], right_ref.at[rows], w_send.at[q, c], w_recv.at[q, c], fsdp=mate
        )

    sqs[me] = jnp.zeros_like(sqs[me])

    def reduce(c, carry):
        to_mate(y, c).wait_recv()
        total = part_ref[rows_of(core, y, c), :].astype(f32) + mbuf[y, c].astype(f32)

        def add(i, acc):
            q = lax.rem(y + 1 + i, ny)
            remote(
                sbuf.at[y, c], ybuf.at[q, c], y_send.at[q, c], y_recv.at[q, c], fsdp=2 * q + core
            ).wait_recv()
            return acc + ybuf[q, c].astype(f32)

        total = lax.fori_loop(0, ny - 1, add, total)
        rows = rows_of(core, y, c)
        right_ref[rows, :] = total.astype(b16)
        sqs[me] = sqs[me] + jnp.sum((total * total).reshape(sub // 8, 8, total.shape[1]), axis=0)

        cross_right(c).start()
        to_other_core(y, c).start()
        return carry

    lax.fori_loop(0, cuts, reduce, 0)

    def to_all(q):
        return remote(
            sqs.at[me], sqs.at[me], sq_send.at[q], sq_recv.at[me], fsdp=q // nt, tp=lax.rem(q, nt)
        )

    def start_squares(i, carry):
        to_all(lax.rem(me + 1 + i, n)).start()
        return carry

    lax.fori_loop(0, n - 1, start_squares, 0)

    def start_spread(i, carry):
        spread(*order(i)).start()
        return carry

    lax.fori_loop(0, (ny - 1) * cuts, start_spread, 0)
    cross_ortho.wait_recv()

    def start_along(i, carry):
        along(lax.rem(t + 1 + i, nt), t).start()
        return carry

    lax.fori_loop(0, nt - 1, start_along, 0)

    def forward(i, carry):
        q, c = order(i)
        rows = rows_of(core, q, c)
        remote(
            right_ref.at[rows], right_ref.at[rows], g_send.at[q, c], g_recv.at[q, c], fsdp=2 * q + core
        ).wait_recv()
        to_other_core(q, c).start()
        return carry

    lax.fori_loop(0, (ny - 1) * cuts, forward, 0)

    def got_square(i, carry):
        q = lax.rem(me + 1 + i, n)
        remote(
            sqs.at[q], sqs.at[q], sq_send.at[q], sq_recv.at[q], fsdp=q // nt, tp=lax.rem(q, nt)
        ).wait_recv()
        return carry

    lax.fori_loop(0, n - 1, got_square, 0)
    total = lax.fori_loop(1, n, lambda q, acc: acc + sqs[q], sqs[0])
    meansq = jnp.sum(total, axis=0, keepdims=True) / cols
    inv_ref[...] = jnp.broadcast_to(lax.rsqrt(meansq + 1e-06), inv_ref.shape)
    cross_inv = across(inv_ref, far_inv, cuts + 1)
    cross_inv.start()

    def finish(i, carry):
        q, c = order(i)
        rows = rows_of(1 - core, q, c)
        remote(
            right_ref.at[rows], right_ref.at[rows], w_send.at[q, c], w_recv.at[q, c], fsdp=mate
        ).wait_recv()
        to_mate(q, c).wait_send()
        to_other_core(q, c).wait_send()

        @pl.when(q != y)
        def _():
            to_peer(q, c).wait_send()
            spread(q, c).wait_send()

        return carry

    lax.fori_loop(0, ny * cuts, finish, 0)

    def drain_squares(i, carry):
        to_all(lax.rem(me + 1 + i, n)).wait_send()
        return carry

    lax.fori_loop(0, n - 1, drain_squares, 0)

    def finish_cross(c, carry):
        cross_right(c).wait()
        return carry

    lax.fori_loop(0, cuts, finish_cross, 0)
    cross_ortho.wait_send()
    cross_inv.wait()

    def finish_along(i, carry):
        q = lax.rem(t + 1 + i, nt)
        along(q, q).wait_recv()
        along(q, t).wait_send()
        return carry

    lax.fori_loop(0, nt - 1, finish_along, 0)


def sub_blocks(quarter):
    for cuts in (4, 2):
        if quarter % (16 * cuts) == 0:
            return cuts
    return 1


def right_sum(part, ortho, nf, nt, cols):
    mine, rank = part.shape
    ny = nf // 2
    quarter = mine // nf
    cuts = sub_blocks(quarter)
    sub = quarter // cuts
    n = nf * nt
    b16, f32 = jnp.bfloat16, jnp.float32
    dma = pltpu.SemaphoreType.DMA
    vmem = pl.BlockSpec(memory_space=pltpu.VMEM)
    return pl.pallas_call(
        functools.partial(right_kernel, nf, nt, cuts, cols),
        out_shape=(
            jax.ShapeDtypeStruct((mine, rank), b16),
            jax.ShapeDtypeStruct((8, rank), f32),
            jax.ShapeDtypeStruct(ortho.shape, b16),
            jax.ShapeDtypeStruct((quarter, rank), b16),
            jax.ShapeDtypeStruct((8, rank), f32),
        ),
        in_specs=[vmem, vmem],
        out_specs=(vmem,) * 5,
        scratch_shapes=[
            pltpu.VMEM((ny, cuts, sub, rank), b16),
            pltpu.VMEM((ny, cuts, sub, rank), b16),
            pltpu.VMEM((ny, cuts, sub, rank), b16),
            pltpu.VMEM((n, 8, rank), f32),
            dma((ny, cuts)), dma((ny, cuts)),
            dma((ny, cuts)), dma((ny, cuts)),
            dma((ny, cuts)), dma((ny, cuts)),
            dma((ny, cuts)), dma((ny, cuts)),
            dma((n,)), dma((n,)),
            dma((cuts + 2,)), dma((cuts + 2,)),
            dma((nt,)), dma((nt,)),
        ],
        compiler_params=pltpu.CompilerParams(
            vmem_limit_bytes=40 << 20, collective_id=1, has_side_effects=True
        ),
        cost_estimate=pl.CostEstimate(
            flops=10_000_000_000, bytes_accessed=4 * mine * rank, transcendentals=0
        ),
        name="right_sum",
    )(part, ortho)


def own_kernel(
    who_ref, w_ref, g_ref, m_ref, ortho_ref, right_ref, inv_ref, new_ref, both_ref, moment_ref, basis_ref
):
    f32 = jnp.float32
    dims = (((1,), (1,)), ((), ()))
    tc = w_ref.shape[2]
    right = right_ref[pl.ds(pl.multiple_of(pl.program_id(0) * tc, tc), tc), :]
    ortho = ortho_ref[...]
    basis = right.astype(f32) * inv_ref[0:1, :]
    basis_ref[0] = basis
    update = lax.dot_general(ortho, basis.astype(jnp.bfloat16), dims, preferred_element_type=f32)
    value = (w_ref[0].astype(f32) - 0.3 * update).astype(jnp.bfloat16)
    new_ref[0] = value
    both_ref[0] = value
    blend = m_ref[0] + g_ref[0].astype(f32)
    moment_ref[0] = blend - 0.05 * lax.dot_general(ortho, right, dims, preferred_element_type=f32)


def apply_own(who, w, g, m, ortho, right, inv):
    _, rows, cols = w.shape
    rank = ortho.shape[1]
    tc = pick(cols, (512, 256, 128))
    spec = pl.BlockSpec((1, rows, tc), lambda j, who: (0, 0, j))
    f32, b16 = jnp.float32, jnp.bfloat16
    return pl.pallas_call(
        own_kernel,
        out_shape=(
            jax.ShapeDtypeStruct((1, rows, cols), b16),
            jax.ShapeDtypeStruct((2, rows, cols), b16),
            jax.ShapeDtypeStruct((1, rows, cols), f32),
            jax.ShapeDtypeStruct((1, cols, rank), f32),
        ),
        grid_spec=pltpu.PrefetchScalarGridSpec(
            num_scalar_prefetch=1,
            grid=(cols // tc,),
            in_specs=[
                spec,
                spec,
                spec,
                pl.BlockSpec(memory_space=pltpu.VMEM),
                pl.BlockSpec(memory_space=pltpu.VMEM),
                pl.BlockSpec(memory_space=pltpu.VMEM),
            ],
            out_specs=(
                spec,
                pl.BlockSpec((1, rows, tc), lambda j, who: (who[0], 0, j)),
                spec,
                pl.BlockSpec((1, tc, rank), lambda j, who: (0, j, 0)),
            ),
        ),
        compiler_params=pltpu.CompilerParams(vmem_limit_bytes=48 << 20),
        cost_estimate=pl.CostEstimate(
            flops=30_000_000_000, bytes_accessed=18 * rows * cols, transcendentals=0
        ),
        name="apply_own",
    )(who, w, g, m, ortho, right, inv)


def other_kernel(nf, who_ref, *refs):
    rights = refs[:nf]
    ortho, w_ref, inv_ref, _, both_ref, base = refs[nf:]
    quarter = rights[0].shape[0]
    f32, b16 = jnp.float32, jnp.bfloat16
    j = pl.program_id(0)

    @pl.when(j == 0)
    def _():
        inv = inv_ref[0:1, :]
        for k, piece in enumerate(rights):
            place = pl.ds(pl.multiple_of(who_ref[1 + k] * quarter, quarter), quarter)
            base[place, :] = (piece[...].astype(f32) * inv).astype(b16)

    tc = w_ref.shape[2]
    update = lax.dot_general(
        ortho[...],
        base[pl.ds(pl.multiple_of(j * tc, tc), tc), :],
        (((1,), (1,)), ((), ())),
        preferred_element_type=f32,
    )
    both_ref[0] = (w_ref[0].astype(f32) - 0.3 * update).astype(b16)


def apply_other(who, rights, ortho, w, inv, both):
    _, rows, cols = w.shape
    rank = inv.shape[1]
    nf = len(rights)
    tc = pick(cols, (512, 256, 128))
    whole = pl.BlockSpec(memory_space=pltpu.VMEM)
    return pl.pallas_call(
        functools.partial(other_kernel, nf),
        out_shape=jax.ShapeDtypeStruct((2, rows, cols), jnp.bfloat16),
        grid_spec=pltpu.PrefetchScalarGridSpec(
            num_scalar_prefetch=1,
            grid=(cols // tc,),
            in_specs=[whole] * (nf + 1)
            + [
                pl.BlockSpec((1, rows, tc), lambda j, who: (0, 0, j)),
                whole,
                pl.BlockSpec(memory_space=pl.ANY),
            ],
            out_specs=pl.BlockSpec((1, rows, tc), lambda j, who: (who[0], 0, j)),
            scratch_shapes=[pltpu.VMEM((cols, rank), jnp.bfloat16)],
        ),
        input_output_aliases={nf + 4: 0},
        compiler_params=pltpu.CompilerParams(vmem_limit_bytes=40 << 20),
        cost_estimate=pl.CostEstimate(
            flops=2 * rows * cols * rank, bytes_accessed=4 * rows * cols, transcendentals=0
        ),
        name="apply_other",
    )(who, *rights, ortho, w, inv, both)


def body(weights, gradient, momentum, basis):
    swap = functools.partial(lax.ppermute, axis_name="rollout", perm=[(0, 1), (1, 0)])
    me = lax.axis_index("rollout")
    f = lax.axis_index("fsdp")
    nf, nt = lax.axis_size("fsdp"), lax.axis_size("tp")
    cols = weights.shape[2] * nt
    weights_other = swap(weights)
    ortho, blend = mid(momentum, gradient, basis, nf, nt)
    partial_right = lax.dot_general(
        blend,
        ortho,
        (((0,), (0,)), ((), ())),
        preferred_element_type=jnp.float32,
    ).astype(jnp.bfloat16)
    right, inv, far_ortho, far_right, inv_other = right_sum(partial_right, ortho, nf, nt, cols)
    ny = nf // 2
    core, y = f % 2, f // 2
    mates = [(i, i ^ 1) for i in range(nf)]
    rights, right_places = [far_right], [core * ny + y]
    for k in range(1, ny):
        rights.append(
            lax.ppermute(far_right, "fsdp", [(i, ((i // 2 - k) % ny) * 2 + i % 2) for i in range(nf)])
        )
        right_places.append(core * ny + (y + k) % ny)
    for k in range(ny):
        rights.append(lax.ppermute(rights[k], "fsdp", mates))
        right_places.append((1 - core) * ny + (y + k) % ny)
    weight_new, both, moment_new, basis_new = apply_own(
        me.reshape(1), weights, gradient, momentum, ortho, right, inv
    )
    who = jnp.stack([1 - me] + right_places).astype(jnp.int32)
    both = apply_other(who, rights, far_ortho, weights_other, inv_other, both)
    return (weight_new, moment_new, basis_new, both)


def solution(mesh):
    return jax.shard_map(
        body,
        mesh=mesh,
        in_specs=(
            P("rollout", "fsdp", "tp"),
            P("rollout", "fsdp", "tp"),
            P("rollout", "fsdp", "tp"),
            P("rollout", "tp", None),
        ),
        out_specs=(
            P("rollout", "fsdp", "tp"),
            P("rollout", "fsdp", "tp"),
            P("rollout", "tp", None),
            P(None, "fsdp", "tp"),
        ),
        check_vma=False,
    )
```
